256 devices in a mesh: gx: 8 (over z), gy: 16 (over x, y), gz: 2 (over core).
Axes of the slice: x: 4, y: 4, z: 8, core: 2. Of those that a mesh axis runs over, the one named last changes fastest.
Arguments:
- panels: float32 [4, 32768], P(None, ('gy', 'gz')), may hold values from -2 to 3, as said below
- diagonal: float32 [32768], P(('gy', 'gz')), may hold values from 0.5 to 2
- right_side: float32 [32, 32768], P(None, ('gy', 'gz')), may hold values from -6 to 6
- start_guess: float32 [32, 32768], P(None, ('gy', 'gz')), may hold values from -6 to 6
Outputs:
- solution: float32 [32, 32768], P(None, ('gy', 'gz'))
- residual: float32 [32, 32768], P(None, ('gy', 'gz'))
- history: float32 [4, 32], replicated
The draws below stay inside these ranges and needn't reach their ends.
Inputs may be any that keep to these rules, and one draw needn't show every extreme that they name: `panels`: rows 0 to 2 are centroids of a closed surface around the anchor, row 3 positive areas between 0.3 and 3.
All inputs are finite; a program needn't handle non-finite values.
Results may differ from the reference program's by a relative error of at most 0.00035.
Values sent between devices are 32-bit elements; how exact they have to be, the bound alone decides.
A program may use at most 64 MiB of HBM per device.

```python
import math
import jax
import jax.numpy as jnp
from jax import lax

N = 32768
NRHS = 32
ITERS = 4


def draw_panels(key, part):
    key_dir = jax.random.fold_in(key, 11)
    key_rad = jax.random.fold_in(key, 12)
    key_area = jax.random.fold_in(key, 13)
    direction = jax.random.normal(key_dir, (3, N), jnp.float32)
    direction = direction / jnp.sqrt(jnp.sum(direction * direction, 0, keepdims=True) + 1e-06)
    radius = 1.0 + 0.2 * jax.random.uniform(key_rad, (1, N), jnp.float32)
    centers = direction * radius
    panel_area = jnp.exp(jax.random.uniform(key_area, (1, N), jnp.float32, jnp.log(0.3), jnp.log(3.0)))
    return jnp.concatenate([centers, panel_area], 0).astype(jnp.float32)


def level_of(rng, shape, cuts, least, largest):
    factor_of = 1.0
    for dim, parts in cuts:
        steps = jax.random.uniform(jax.random.fold_in(jax.random.fold_in(rng, 6), dim), (parts,), jnp.float32, least / len(cuts), largest / len(cuts))
        factor_of = factor_of * jnp.repeat(jnp.exp(steps), shape[dim] // parts).reshape((-1,) + (1,) * (len(shape) - 1 - dim))
    return factor_of


def scatter_about(key, shape, spread, bound, shards=(), dtype=jnp.bfloat16):
    drawn = spread * jax.random.normal(key, shape, jnp.float32)
    if shards:
        drawn = drawn * level_of(key, shape, shards, -0.22, 0.18)
    return jnp.clip(drawn, -bound, bound).astype(dtype)


def setup_inputs(seed: int = 0) -> dict:
    arg_keys = jax.random.split(jax.random.key(seed), 5)
    panels = draw_panels(jax.random.fold_in(arg_keys[4], 71), 0)
    diagonal = jnp.clip(jnp.exp(math.log(2.0) - 1.3862944 * jax.random.uniform(arg_keys[1], (N,), jnp.float32) ** level_of(arg_keys[1], (N,), ((0, 32),), -0.2, 0.2)), 0.5, 2.0)
    right_side = scatter_about(arg_keys[2], (NRHS, N), 1.0, 6.0, ((1, 32),), jnp.float32)
    start_guess = scatter_about(arg_keys[3], (NRHS, N), 1.0, 6.0, ((1, 32),), jnp.float32)
    return {"panels": panels, "diagonal": diagonal, "right_side": right_side, "start_guess": start_guess}


soft_sq = 0.0025

def kernel(row_pan, col_pan):
    dist_sq = (row_pan[0][:, None] - col_pan[0][None, :]) ** 2
    dist_sq = dist_sq + (row_pan[1][:, None] - col_pan[1][None, :]) ** 2
    dist_sq = dist_sq + (row_pan[2][:, None] - col_pan[2][None, :]) ** 2
    weight = (row_pan[3] * N ** (-0.5))[:, None] * col_pan[3][None, :]
    return weight * lax.rsqrt(dist_sq + soft_sq)

def apply_operator(panels, diagonal, vector):
    row_len = min(N, 1024)
    blocks = panels.reshape(4, N // row_len, row_len).transpose(1, 0, 2)

    def one_block(row_pan):
        return lax.dot_general(vector, kernel(row_pan, panels), (((1,), (1,)), ((), ())), precision=lax.Precision.HIGHEST)
    products = lax.map(one_block, blocks)
    products = products.transpose(1, 0, 2).reshape(vector.shape[0], N)
    return diagonal[None, :] * vector + products

def reference(panels, diagonal, right_side, start_guess):
    residual = right_side - apply_operator(panels, diagonal, start_guess)
    image_res = apply_operator(panels, diagonal, residual)
    solution = start_guess
    direction = jnp.zeros_like(residual)
    sdir = jnp.zeros_like(residual)
    zdir = jnp.zeros_like(residual)
    gamma_prev = jnp.ones((NRHS,), jnp.float32)
    alpha_prev = jnp.ones((NRHS,), jnp.float32)
    records = []
    for turn_index in range(ITERS):
        gamma_now = lax.optimization_barrier(jnp.sum(residual * residual, 1))
        delta_now = lax.optimization_barrier(jnp.sum(image_res * residual, 1))
        omega_now = lax.optimization_barrier(jnp.sum(image_res * image_res, 1))
        fresh = apply_operator(panels, diagonal, image_res)
        records.append(jnp.sqrt(omega_now / gamma_now))
        if turn_index == 0:
            beta_now = jnp.zeros((NRHS,), jnp.float32)
            alpha_now = gamma_now / delta_now
        else:
            beta_now = gamma_now / gamma_prev
            alpha_now = gamma_now / (delta_now - beta_now * gamma_now / alpha_prev)
        beta_col = beta_now[:, None]
        alpha_col = alpha_now[:, None]
        zdir = fresh + beta_col * zdir
        sdir = image_res + beta_col * sdir
        direction = residual + beta_col * direction
        solution = solution + alpha_col * direction
        residual = residual - alpha_col * sdir
        image_res = image_res - alpha_col * zdir
        gamma_prev = gamma_now
        alpha_prev = alpha_now
    return (solution, residual, jnp.stack(records))
```

```python
import functools
import jax
import jax.numpy as jnp
from jax import lax
from jax.experimental import pallas as pl
from jax.experimental.pallas import tpu as pltpu
from jax.sharding import PartitionSpec as P

ITERS = 4
SOFT_SQ = 0.0025
LANE = 128
MESH = pl.DeviceIdType.MESH
F32 = jnp.float32
BF16 = jnp.bfloat16


def cg_kernel(np_, ngy, ngz, cases, chunk,
              panels, diagonal, right, start, sol_out, res_out, hist_out,
              rowpan, coords, ghi, glo, vp, vg, cz, ps, rs, acc, acc_lo,
              sol_c, r_c, s_c, d_c, r_r, s_r, zdir, gprev, aprev, hist, scal,
              dtile, dplane, dsum, dz,
              pan_s, pan_r, ag_s, ag_r, z_s, z_r, rs_s, rs_r, dp_s, dp_r, dz_s, dz_r):
    nq = ngy * ngz
    total = nq * np_ * LANE
    inv_root = total ** -0.5
    p = lax.axis_index("gx")
    gy = lax.axis_index("gy")
    gz = lax.axis_index("gz")
    q = gy * ngz + gz
    own = pl.ds(pl.multiple_of(p * LANE, LANE), LANE)
    span = 2 * LANE * chunk
    per_chunk = 2 * chunk
    lane = lax.broadcasted_iota(jnp.int32, (cases, LANE), 1)
    lane8 = lax.broadcasted_iota(jnp.int32, (8, LANE), 1)
    groups = cases // 8

    def plane_dev(k):
        other = lax.rem(q + k, nq)
        return other, (p, other // ngz, lax.rem(other, ngz))

    def z_dev(k):
        other = lax.rem(p + k, np_)
        return other, (other, gy, gz)

    def plane_copy(k, src, dst_of, send, recv_of):
        other, dev = plane_dev(k)
        out = pltpu.make_async_remote_copy(src, dst_of(q), send.at[k], recv_of(q), device_id=dev, device_id_type=MESH)
        inc = pltpu.make_async_remote_copy(src, dst_of(other), send.at[k], recv_of(other), device_id=dev, device_id_type=MESH)
        return out, inc

    def z_copy(k, src_of, dst_of, send, recv_of):
        other, dev = z_dev(k)
        out = pltpu.make_async_remote_copy(src_of(other), dst_of(p), send.at[k], recv_of(p), device_id=dev, device_id_type=MESH)
        inc = pltpu.make_async_remote_copy(src_of(other), dst_of(other), send.at[k], recv_of(other), device_id=dev, device_id_type=MESH)
        return out, inc

    def loop(lo, hi, fn):
        def step(i, carry):
            fn(i)
            return carry
        lax.fori_loop(lo, hi, step, 0)

    pan_copy = lambda k: plane_copy(k, panels.at[:, own], lambda s: rowpan.at[s], pan_s, lambda s: pan_r.at[s])
    ag_copy = lambda k, buf: plane_copy(k, vp, lambda s: vg.at[buf, s], ag_s, lambda s: ag_r.at[buf, s])
    zg_copy = lambda k, par: z_copy(k, lambda o: vp, lambda s: cz.at[par, s], z_s, lambda s: z_r.at[par, s])
    rs_copy = lambda k, par: z_copy(k, lambda o: ps.at[o], lambda s: rs.at[par, s], rs_s, lambda s: rs_r.at[par, s])
    dp_copy = lambda k: plane_copy(k, dtile, lambda s: dplane.at[s], dp_s, lambda s: dp_r.at[s])
    dz_copy = lambda k: z_copy(k, lambda o: dsum, lambda s: dz.at[s], dz_s, lambda s: dz_r.at[s])

    barrier = pltpu.get_barrier_semaphore()
    loop(1, nq, lambda k: pl.semaphore_signal(barrier, inc=1, device_id=plane_dev(k)[1], device_id_type=MESH))
    loop(1, np_, lambda k: pl.semaphore_signal(barrier, inc=1, device_id=z_dev(k)[1], device_id_type=MESH))
    vp[...] = start[:, own]
    pl.semaphore_wait(barrier, nq + np_ - 2)

    loop(1, nq, lambda k: pan_copy(k)[0].start())
    loop(1, nq, lambda k: ag_copy(k, 0)[0].start())
    rowpan[q] = panels[:, own]
    vg[0, q] = vp[...]
    ps[...] = jnp.zeros_like(ps)
    for s in range(np_):
        sol_c[s] = start[:, s * LANE:(s + 1) * LANE]
    s_c[...] = jnp.zeros_like(s_c)
    d_c[...] = jnp.zeros_like(d_c)
    r_c[...] = jnp.zeros_like(r_c)
    s_r[...] = jnp.zeros_like(s_r)
    r_r[...] = jnp.zeros_like(r_r)
    zdir[...] = jnp.zeros_like(zdir)
    gprev[...] = jnp.ones_like(gprev)
    aprev[...] = jnp.ones_like(aprev)
    hist[...] = jnp.zeros_like(hist)

    def build(slot):
        part = lax.div(slot, per_chunk)
        base = lax.rem(slot, per_chunk) * LANE
        for axis in range(3):
            coords[axis] = jnp.broadcast_to(rowpan[slot, axis:axis + 1, :], (LANE, LANE)).T
        rows_at = 32

        def block(i):
            here = pl.ds(pl.multiple_of(i * rows_at, rows_at), rows_at)
            there = pl.ds(pl.multiple_of(base + i * rows_at, rows_at), rows_at)
            x, y, z = coords[0, here, :], coords[1, here, :], coords[2, here, :]
            for ct in range(np_):
                cols = slice(ct * LANE, (ct + 1) * LANE)
                dx = x - panels[0:1, cols]
                dy = y - panels[1:2, cols]
                dzz = z - panels[2:3, cols]
                value = lax.rsqrt(dx * dx + dy * dy + dzz * dzz + SOFT_SQ)
                top = value.astype(BF16)
                ghi[part, there, cols] = top
                glo[part, there, cols] = (value - top.astype(F32)).astype(BF16)
        loop(0, LANE // rows_at, block)

    build(q)

    def build_other(k):
        pan_copy(k)[1].wait_recv()
        build(plane_dev(k)[0])
    loop(1, nq, build_other)
    loop(1, nq, lambda k: pan_copy(k)[0].wait_send())

    def pack_dots(sums):
        tile = jnp.zeros((8, LANE), F32)
        for d in range(3):
            for g in range(groups):
                tile = jnp.where(lane8 == groups * d + g, sums[d][8 * g:8 * g + 8, :], tile)
        return tile

    def unpack_dots(tile):
        out = []
        for d in range(3):
            out.append(jnp.concatenate([tile[:, groups * d + g:groups * d + g + 1] for g in range(groups)], 0))
        return out

    def row_sum(value):
        return jnp.sum(value, axis=1, keepdims=True)

    def coefficients(tile, turn):
        gamma, delta, omega = unpack_dots(tile)
        hist[...] = jnp.where(lane == turn, jnp.sqrt(omega / gamma), hist[...])
        gamma_prev = gprev[:, 0:1]
        alpha_prev = aprev[:, 0:1]
        beta = jnp.where(turn == 0, 0.0, gamma / gamma_prev)
        alpha = gamma / (delta - beta * gamma / alpha_prev)
        gprev[...] = jnp.broadcast_to(gamma, (cases, LANE))
        aprev[...] = jnp.broadcast_to(alpha, (cases, LANE))
        scal[...] = jnp.broadcast_to(beta, (cases, LANE))
        return alpha, beta

    def event(e, carry):
        par = lax.rem(e, 2)
        nxt = 1 - par
        turn = lax.rem(e, 3)
        after = lax.rem(e + 1, 3)
        loop(1, nq, lambda k: ag_copy(k, turn)[1].wait_recv())

        def matmul(c):
            pieces = []
            for i in range(per_chunk):
                slot = c * per_chunk + i
                value = vg[turn, slot] * (rowpan[slot, 3:4, :] * inv_root)
                top = value.astype(BF16)
                value = value - top.astype(F32)
                mid = value.astype(BF16)
                low = (value - mid.astype(F32)).astype(BF16)
                pieces.append(jnp.concatenate([top, mid, low], 0))
            lhs = jnp.concatenate(pieces, 1)
            main = jnp.dot(lhs, ghi[c], preferred_element_type=F32)
            rest = jnp.dot(lhs[:2 * cases], glo[c], preferred_element_type=F32)
            small = main[2 * cases:] + rest[cases:]
            acc[...] += main[:cases] + (main[cases:2 * cases] + rest[:cases] + small)

        acc[...] = jnp.zeros_like(acc)
        loop(0, nq // per_chunk, matmul)
        for s in range(np_):
            ps[s, 0:cases, :] = acc[:, s * LANE:(s + 1) * LANE]

        @pl.when(e >= 2)
        def _():
            def add(s, sums):
                r = r_r[s]
                a = vg[turn, s]
                return sums[0] + r * r, sums[1] + a * r, sums[2] + a * a
            zero = jnp.zeros((cases, LANE), F32)
            sums = lax.fori_loop(0, nq, add, (zero, zero, zero))
            tile = pack_dots([row_sum(v) for v in sums])
            for s in range(np_):
                ps[s, cases:, :] = tile

        loop(1, np_, lambda k: rs_copy(k, par)[0].start())
        rs[par, p] = ps[p]
        loop(1, nq, lambda k: ag_copy(k, turn)[0].wait_send())

        @pl.when(e > 0)
        def _():
            loop(1, np_, lambda k: zg_copy(k, par)[0].wait_send())
            cz[par, p] = vp[...]
        loop(1, np_, lambda k: rs_copy(k, par)[1].wait_recv())
        got = rs[par, 0]
        for s in range(1, np_):
            got = got + rs[par, s]
        fresh = got[:cases] * panels[3:4, own] + diagonal[0:1, own] * vp[...]

        @pl.when(e == 0)
        def _():
            vp[...] = right[:, own] - fresh

        @pl.when(e == 1)
        def _():
            vp[...] = fresh

        @pl.when(e >= 2)
        def _():
            alpha, beta = coefficients(got[cases:], e - 2)
            z = fresh + beta * zdir[...]
            zdir[...] = z
            vp[...] = vp[...] - alpha * z

        vg[after, q] = vp[...]

        @pl.when(e < ITERS)
        def _():
            loop(1, nq, lambda k: ag_copy(k, after)[0].start())
        loop(1, np_, lambda k: zg_copy(k, nxt)[0].start())
        loop(1, np_, lambda k: rs_copy(k, par)[0].wait_send())

        @pl.when(e > 0)
        def _():
            loop(1, np_, lambda k: zg_copy(k, par)[1].wait_recv())

        @pl.when(e == 1)
        def _():
            loop(0, nq, lambda s: r_r.__setitem__(s, vg[turn, s]))
            loop(0, np_, lambda s: r_c.__setitem__(s, cz[par, s]))

        @pl.when(e >= 2)
        def _():
            alpha = aprev[...]
            beta = scal[...]

            def rows(s):
                step = vg[turn, s] + beta * s_r[s]
                s_r[s] = step
                r_r[s] = r_r[s] - alpha * step
            loop(0, nq, rows)

            def cols(s):
                step = cz[par, s] + beta * s_c[s]
                s_c[s] = step
                along = r_c[s] + beta * d_c[s]
                d_c[s] = along
                sol_c[s] = sol_c[s] + alpha * along
                r_c[s] = r_c[s] - alpha * step
            loop(0, np_, cols)
        return carry

    lax.fori_loop(0, ITERS + 1, event, 0)

    last = (ITERS + 1) % 2
    r = r_c[p]
    a = vp[...]
    dtile[...] = pack_dots([row_sum(r * r), row_sum(a * r), row_sum(a * a)])
    loop(1, nq, lambda k: dp_copy(k)[0].start())
    dplane[q] = dtile[...]
    cz[last, p] = vp[...]
    loop(1, nq, lambda k: dp_copy(k)[1].wait_recv())
    dsum[...] = jnp.sum(dplane[...], axis=0)
    loop(1, np_, lambda k: dz_copy(k)[0].start())
    dz[p] = dsum[...]
    loop(1, nq, lambda k: dp_copy(k)[0].wait_send())
    loop(1, np_, lambda k: zg_copy(k, last)[0].wait_send())
    loop(1, np_, lambda k: zg_copy(k, last)[1].wait_recv())
    loop(1, np_, lambda k: dz_copy(k)[1].wait_recv())
    alpha, beta = coefficients(jnp.sum(dz[...], axis=0), ITERS - 1)
    for s in range(np_):
        cols = slice(s * LANE, (s + 1) * LANE)
        step = cz[last, s] + beta * s_c[s]
        along = r_c[s] + beta * d_c[s]
        sol_out[:, cols] = sol_c[s] + alpha * along
        res_out[:, cols] = r_c[s] - alpha * step
    hist_out[...] = hist[...].T[0:ITERS, :]
    loop(1, np_, lambda k: dz_copy(k)[0].wait_send())


def on_device(np_, ngy, ngz, panels, diagonal, right, start):
    nq = ngy * ngz
    cases, cols = right.shape
    chunk = min(4, nq // 2)
    span = 2 * LANE * chunk
    parts = nq // (2 * chunk)
    vm = lambda *shape: pltpu.VMEM(shape, F32)
    dma = lambda *shape: pltpu.SemaphoreType.DMA(shape)
    state = (np_, cases, LANE)
    wide = (nq, cases, LANE)
    one = (cases, LANE)
    scratch = [
        vm(nq, 4, LANE), vm(3, LANE, LANE),
        pltpu.VMEM((parts, span, cols), BF16), pltpu.VMEM((parts, span, cols), BF16),
        vm(*one), vm(3, *wide), vm(2, *state), vm(np_, cases + 8, LANE), vm(2, np_, cases + 8, LANE),
        vm(cases, cols), vm(8, LANE),
        vm(*state), vm(*state), vm(*state), vm(*state), vm(*wide), vm(*wide),
        vm(*one), vm(*one), vm(*one), vm(*one), vm(*one),
        vm(8, LANE), vm(nq, 8, LANE), vm(8, LANE), vm(np_, 8, LANE),
        dma(nq), dma(nq), dma(nq), dma(3, nq), dma(np_), dma(2, np_), dma(np_), dma(2, np_),
        dma(nq), dma(nq), dma(np_), dma(np_),
    ]
    return pl.pallas_call(
        functools.partial(cg_kernel, np_, ngy, ngz, cases, chunk),
        out_shape=(
            jax.ShapeDtypeStruct((cases, cols), F32),
            jax.ShapeDtypeStruct((cases, cols), F32),
            jax.ShapeDtypeStruct((ITERS, cases), F32),
        ),
        in_specs=[pl.BlockSpec(memory_space=pltpu.VMEM)] * 4,
        out_specs=tuple([pl.BlockSpec(memory_space=pltpu.VMEM)] * 3),
        scratch_shapes=scratch,
        compiler_params=pltpu.CompilerParams(
            collective_id=0, has_side_effects=True, vmem_limit_bytes=48 * 1024 * 1024
        ),
        name="cg",
    )(panels, diagonal[None, :], right, start)


def solution(mesh):
    cut = P(None, ("gy", "gz"))
    sizes = dict(mesh.shape)
    return jax.shard_map(
        functools.partial(on_device, sizes["gx"], sizes["gy"], sizes["gz"]),
        mesh=mesh,
        in_specs=(cut, P(("gy", "gz")), cut, cut),
        out_specs=(cut, cut, P()),
        check_vma=False,
    )
```

```python
import functools
import math
import jax
import jax.numpy as jnp
from jax import lax
from jax.experimental import pallas as pl
from jax.experimental.pallas import tpu as pltpu
from jax.sharding import PartitionSpec as P

ITERS = 4
SOFT_SQ = 0.0025
LANE = 128
MESH = pl.DeviceIdType.MESH
F32 = jnp.float32
BF16 = jnp.bfloat16


def ring_distance(step, size):
    return min(step, size - step)


def chip_offsets(side):
    every = [(dx, dy) for dx in range(side) for dy in range(side)]
    return sorted(every, key=lambda o: (ring_distance(o[0], side) + ring_distance(o[1], side), o))


def send_order(side):
    hops = [ring_distance(dx, side) + ring_distance(dy, side) for dx, dy in chip_offsets(side)]
    near = [k for k in range(1, len(hops)) if hops[k] == 1]
    return near, list(range(len(hops) - 1, len(near), -1))


def arrival_order(side):
    near, rest = send_order(side)
    first = [(0, 0), (0, 1)]
    return first + [(k, c) for part in (near, rest) for c in range(2) for k in part]


def cg_kernel(np_, ngy, cases, per_chunk,
              panels_hbm, diagonal_hbm, right_hbm, start_hbm, sol_out, res_out, hist_out,
              panels, diagonal, right, start, rowpan, ghi, glo, rhs, lhs_last, vp, vg, cz, ps, rs, dots_out, dots_in, acc,
              sol_c, r_c, s_c, d_c, r_r, s_r, zdir, gprev, aprev, hist, scal, sums, dtile, dplane, dsum, dz,
              in_s, pan_s, pan_r, ag_s, ag_r, z_s, z_r, rs_s, rs_r, dt_s, dt_r, dp_s, dp_r, dz_s, dz_r):
    side = math.isqrt(ngy)
    offsets = chip_offsets(side)
    order = arrival_order(side)
    place = {slot: i for i, slot in enumerate(order)}
    nslot = len(order)
    nchunk = nslot // per_chunk
    inv_root = (nslot * np_ * LANE) ** -0.5
    p = lax.axis_index("gx")
    gy = lax.axis_index("gy")
    gz = lax.axis_index("gz")
    x, y = gy // side, lax.rem(gy, side)
    own = pl.ds(pl.multiple_of(p * LANE, LANE), LANE)
    lane = lax.broadcasted_iota(jnp.int32, (cases, LANE), 1)
    lane8 = lax.broadcasted_iota(jnp.int32, (8, LANE), 1)
    row8 = lax.broadcasted_iota(jnp.int32, (8, LANE), 0)
    groups = cases // 8
    far_z = sorted(range(1, np_), key=lambda d: -ring_distance(d, np_))
    near, rest = send_order(side)
    far_chip = near + rest

    def chip_at(k, sign):
        dx, dy = offsets[k]
        if sign < 0:
            dx, dy = (side - dx) % side, (side - dy) % side
        return lax.rem(x + dx, side) * side + lax.rem(y + dy, side)

    def chip(k, core):
        return (p, chip_at(k, -1), gz if core == 0 else 1 - gz)

    def z_of(d):
        return lax.rem(p + d, np_)

    def z_dev(d):
        return (z_of(d), gy, gz)

    def remote(src, dst, send, recv, dev):
        return pltpu.make_async_remote_copy(src, dst, send, recv, device_id=dev, device_id_type=MESH)

    def loop(lo, hi, fn):
        def step(i, carry):
            fn(i)
            return carry
        lax.fori_loop(lo, hi, step, 0)

    def everyone_copy(k, core, src, dst, send, recv):
        i = place[k, core]
        return remote(src, dst.at[i], send.at[i], recv.at[i], chip(k, core))

    peers = [s for s in order if s != (0, 0)]

    def ag_copy(k, core, buf):
        i = place[k, core]
        return remote(vp, vg.at[buf, i], ag_s.at[i], ag_r.at[buf, i], chip(k, core))

    def relay_copy(k, buf):
        i, j = place[k, 0], place[k, 1]
        return remote(vg.at[buf, i], vg.at[buf, j], ag_s.at[j], ag_r.at[buf, j], (p, gy, 1 - gz))

    def zg_send(d, par):
        return remote(vp, cz.at[par, p], z_s.at[d], z_r.at[par, p], z_dev(d))

    def zg_recv(d, par):
        o = z_of(d)
        return remote(vp, cz.at[par, o], z_s.at[d], z_r.at[par, o], z_dev(d))

    def rs_copy(d, par):
        return remote(ps.at[z_of(d)], rs.at[par, d], rs_s.at[d], rs_r.at[par, d], z_dev(d))

    def dt_copy(d, par):
        return remote(dots_out, dots_in.at[par, d], dt_s.at[d], dt_r.at[par, d], z_dev(d))

    def dz_copy(d):
        return remote(dsum, dz.at[d], dz_s.at[d], dz_r.at[d], z_dev(d))

    loads = [
        pltpu.make_async_copy(panels_hbm, panels, in_s.at[0]),
        pltpu.make_async_copy(start_hbm.at[:, own], vp, in_s.at[1]),
        pltpu.make_async_copy(start_hbm, start, in_s.at[2]),
        pltpu.make_async_copy(right_hbm, right, in_s.at[3]),
        pltpu.make_async_copy(diagonal_hbm, diagonal, in_s.at[4]),
    ]
    for load in loads:
        load.start()

    barrier = pltpu.get_barrier_semaphore()
    for k, core in reversed(peers):
        pl.semaphore_signal(barrier, inc=1, device_id=chip(k, core), device_id_type=MESH)
    for d in far_z:
        pl.semaphore_signal(barrier, inc=1, device_id=z_dev(d), device_id_type=MESH)

    loads[0].wait()
    rowpan[0] = panels[:, own]

    def split(value):
        top = value.astype(BF16).astype(F32)
        mid = (value - top).astype(BF16).astype(F32)
        return top, mid, value - top - mid

    row_n = lax.broadcasted_iota(jnp.int32, (8, LANE), 0)
    for s in range(np_):
        cols = slice(s * LANE, (s + 1) * LANE)
        ax, ay, at = (panels[i:i + 1, cols] for i in range(3))
        other = jnp.where(row_n == 4, 1.0, jnp.where(row_n == 5, ax * ax + ay * ay + at * at, 0.0))
        for i, value in enumerate((ax, ay, at)):
            other = jnp.where(row_n == i, -2.0 * value, other)
        top, mid, low = split(other)
        rhs[:, cols] = jnp.concatenate([top, mid, low, top, mid, top], 0).astype(BF16)

    for load in loads[1:]:
        load.wait()
    vg[0, 0] = vp[...]
    for s in range(np_):
        sol_c[s] = start[:, s * LANE:(s + 1) * LANE]
    dots_out[...] = jnp.zeros_like(dots_out)
    s_c[...] = jnp.zeros_like(s_c)
    d_c[...] = jnp.zeros_like(d_c)
    r_c[...] = jnp.zeros_like(r_c)
    s_r[...] = jnp.zeros_like(s_r)
    r_r[...] = jnp.zeros_like(r_r)
    zdir[...] = jnp.zeros_like(zdir)
    gprev[...] = jnp.ones_like(gprev)
    aprev[...] = jnp.ones_like(aprev)
    hist[...] = jnp.zeros_like(hist)

    with jax.named_scope("barrier"):
        pl.semaphore_wait(barrier, nslot - 1 + np_ - 1)
    def pan_copy(k, core):
        return everyone_copy(k, core, panels.at[:, own], rowpan, pan_s, pan_r)

    for k, core in sorted(peers, key=lambda s: -s[0]):
        pan_copy(k, core).start()

    def send_piece(buf):
        for k in far_chip:
            ag_copy(k, 0, buf).start()
        ag_copy(0, 1, buf).start()

    send_piece(0)

    def build(c):
        for n, (k, core) in enumerate(order[c * per_chunk:(c + 1) * per_chunk]):
            i = c * per_chunk + n
            pan = rowpan[i]
            ax, ay, at = (pan[j:j + 1] for j in range(3))
            tile = jnp.where(row8 == 4, ax * ax + ay * ay + at * at + SOFT_SQ, jnp.where(row8 == 5, 1.0, 0.0))
            for j, value in enumerate((ax, ay, at)):
                tile = jnp.where(row8 == j, value, tile)
            top, mid, low = split(tile)
            lhs = jnp.concatenate([top, top, top, mid, mid, low], 0).T.astype(BF16)
            there = slice(n * LANE, (n + 1) * LANE)
            for t in range(np_ * LANE // width):
                cols = slice(t * width, (t + 1) * width)
                value = lax.rsqrt(jnp.dot(lhs, rhs[:, cols], preferred_element_type=F32))
                top = value.astype(BF16)
                ghi[c, there, cols] = top
                glo[c, there, cols] = (value - top.astype(F32)).astype(BF16)

    width = 2 * LANE

    def pack_dots(parts):
        out = jnp.zeros((8, LANE), F32)
        for d in range(3):
            for g in range(groups):
                out = jnp.where(lane8 == groups * d + g, parts[d][8 * g:8 * g + 8, :], out)
        return out

    def unpack_dots(got):
        out = []
        for d in range(3):
            out.append(jnp.concatenate([got[:, groups * d + g:groups * d + g + 1] for g in range(groups)], 0))
        return out

    def row_sum(value):
        return jnp.sum(value, axis=1, keepdims=True)

    def coefficients(got, turn):
        gamma, delta, omega = unpack_dots(got)
        hist[...] = jnp.where(lane == turn, jnp.sqrt(omega / gamma), hist[...])
        gamma_prev = gprev[:, 0:1]
        alpha_prev = aprev[:, 0:1]
        beta = jnp.where(turn == 0, 0.0, gamma / gamma_prev)
        alpha = gamma / (delta - beta * gamma / alpha_prev)
        gprev[...] = jnp.broadcast_to(gamma, (cases, LANE))
        aprev[...] = jnp.broadcast_to(alpha, (cases, LANE))
        scal[...] = jnp.broadcast_to(beta, (cases, LANE))
        return alpha, beta

    def rows_of(c, buf):
        pieces = []
        for i in range(c * per_chunk, (c + 1) * per_chunk):
            value = vg[buf, i] * (rowpan[i, 3:4, :] * inv_root)
            top = value.astype(BF16)
            value = value - top.astype(F32)
            mid = value.astype(BF16)
            low = (value - mid.astype(F32)).astype(BF16)
            pieces.append(jnp.concatenate([top, mid, low], 0))
        return jnp.concatenate(pieces, 1)

    def product(lhs, top, low):
        main = jnp.dot(lhs, top, preferred_element_type=F32)
        rest = jnp.dot(lhs[:2 * cases], low, preferred_element_type=F32)
        small = main[2 * cases:] + rest[cases:]
        return main[:cases] + (main[cases:2 * cases] + rest[:cases] + small)

    def matmul(c, buf):
        part = product(rows_of(c, buf), ghi[c], glo[c])
        acc[...] = part if c == 0 else part + acc[...]

    def last_matmul(buf, par):
        c = nchunk - 1
        lhs_last[...] = rows_of(c, buf)
        half = np_ // 2
        for turn in (1, 0):
            j = lax.rem(lax.div(p, half) + turn, 2)
            cols = pl.ds(pl.multiple_of(j * (half * LANE), half * LANE), half * LANE)
            part = acc[:, cols] + product(lhs_last[...], ghi[c, :, cols], glo[c, :, cols])
            for h in range(half):
                ps[half * j + h] = part[:, h * LANE:(h + 1) * LANE]
            for h in range(half):
                to = half * j + h
                d = lax.rem(to + np_ - p, np_)

                @pl.when(d > 0)
                def _():
                    remote(ps.at[to], rs.at[par, d], rs_s.at[d], rs_r.at[par, d], (to, gy, gz)).start()

    def dots(first, stop, buf, parts):
        g, d, o = parts
        for i in range(first, stop):
            r, a = r_r[i], vg[buf, i]
            g, d, o = g + r * r, d + a * r, o + a * a
        return g, d, o

    def arrive(c, buf):
        with jax.named_scope(f"ag_wait{c}"):
            need = order[c * per_chunk:(c + 1) * per_chunk]
            direct = [k for k, core in need if core == 0 and k > 0]
            if c == 1:
                direct = [k for k in far_chip if place[k, 0] >= per_chunk]
            elif c > 1:
                direct = []
            for k in direct:
                ag_copy(k, 0, buf).wait_recv()
                relay_copy(k, buf).start()
            for k, core in need:
                if core == 1:
                    ag_copy(k, 1, buf).wait_recv()

    with jax.named_scope("build"):
        for c in range(nchunk):
            with jax.named_scope(f"pan_wait{c}"):
                for k, core in order[c * per_chunk:(c + 1) * per_chunk]:
                    if (k, core) != (0, 0):
                        pan_copy(k, core).wait_recv()
            if c > 0:
                arrive(c - 1, 0)
            build(c)
            if c > 0:
                matmul(c - 1, 0)
        arrive(nchunk - 1, 0)
    for k, core in peers:
        pan_copy(k, core).wait_send()

    def event(e, carry):
        par = lax.rem(e, 2)
        nxt = 1 - par
        buf = lax.rem(e, 3)
        after = lax.rem(e + 1, 3)
        @pl.when(e > 0)
        def _():
            for c in range(nchunk - 1):
                arrive(c, buf)
                if c == nchunk - 2:
                    arrive(c + 1, buf)
                with jax.named_scope(f"matmul{c}"):
                    matmul(c, buf)
                    parts = (sums[0], sums[1], sums[2])
                    if c == 0:
                        parts = (jnp.zeros((cases, LANE), F32),) * 3
                    stop = (c + 1) * per_chunk if c < nchunk - 2 else nslot
                    parts = dots(c * per_chunk, stop, buf, parts)
                    if c < nchunk - 2:
                        sums[0], sums[1], sums[2] = parts
                    else:
                        dots_out[...] = pack_dots([row_sum(v) for v in parts])
            for d in far_z:
                dt_copy(d, par).start()
        with jax.named_scope("matmul3"):
            last_matmul(buf, par)
        dots_in[par, 0] = dots_out[...]
        rs[par, 0] = ps[p]
        for k in far_chip:
            ag_copy(k, 0, buf).wait_send()
            relay_copy(k, buf).wait_send()
        ag_copy(0, 1, buf).wait_send()

        @pl.when(e > 0)
        def _():
            for d in far_z:
                zg_send(d, par).wait_send()
            cz[par, p] = vp[...]
        with jax.named_scope("rs_wait"):
            @pl.when(e > 0)
            def _():
                for d in far_z:
                    dt_copy(d, par).wait_recv()
            for d in far_z:
                rs_copy(d, par).wait_recv()
        got = jnp.sum(rs[par], axis=0)
        fresh = got * panels[3:4, own] + diagonal[0:1, own] * vp[...]

        @pl.when(e == 0)
        def _():
            vp[...] = right[:, own] - fresh

        @pl.when(e == 1)
        def _():
            vp[...] = fresh

        @pl.when(e >= 2)
        def _():
            alpha, beta = coefficients(jnp.sum(dots_in[par], axis=0), e - 2)
            z = fresh + beta * zdir[...]
            zdir[...] = z
            vp[...] = vp[...] - alpha * z

        @pl.when(e < ITERS)
        def _():
            send_piece(after)
        for d in far_z:
            zg_send(d, nxt).start()
        vg[after, 0] = vp[...]
        with jax.named_scope("rs_send"):
            for d in far_z:
                rs_copy(d, par).wait_send()

        @pl.when(e > 0)
        def _():
            for d in far_z:
                dt_copy(d, par).wait_send()
            for d in far_z:
                zg_recv(d, par).wait_recv()

        @pl.when(e == 1)
        def _():
            loop(0, nslot, lambda s: r_r.__setitem__(s, vg[buf, s]))
            loop(0, np_, lambda s: r_c.__setitem__(s, cz[par, s]))

        @pl.when(e >= 2)
        def _():
            alpha = aprev[...]
            beta = scal[...]

            def rows(s):
                step = vg[buf, s] + beta * s_r[s]
                s_r[s] = step
                r_r[s] = r_r[s] - alpha * step
            loop(0, nslot, rows)

            def cols(s):
                step = cz[par, s] + beta * s_c[s]
                s_c[s] = step
                along = r_c[s] + beta * d_c[s]
                d_c[s] = along
                sol_c[s] = sol_c[s] + alpha * along
                r_c[s] = r_c[s] - alpha * step
            loop(0, np_, cols)
        return carry

    lax.fori_loop(0, ITERS + 1, event, 0)

    last = (ITERS + 1) % 2
    r = r_c[p]
    a = vp[...]
    dtile[...] = pack_dots([row_sum(r * r), row_sum(a * r), row_sum(a * a)])
    for k, core in reversed(peers):
        everyone_copy(k, core, dtile, dplane, dp_s, dp_r).start()
    dplane[0] = dtile[...]
    cz[last, p] = vp[...]
    with jax.named_scope("dp_wait"):
        for k, core in peers:
            everyone_copy(k, core, dtile, dplane, dp_s, dp_r).wait_recv()
    dsum[...] = jnp.sum(dplane[...], axis=0)
    for d in far_z:
        dz_copy(d).start()
    dz[0] = dsum[...]
    for k, core in peers:
        everyone_copy(k, core, dtile, dplane, dp_s, dp_r).wait_send()
    for d in far_z:
        zg_send(d, last).wait_send()
    with jax.named_scope("dz_wait"):
        for d in far_z:
            zg_recv(d, last).wait_recv()
        for d in far_z:
            dz_copy(d).wait_recv()
    alpha, beta = coefficients(jnp.sum(dz[...], axis=0), ITERS - 1)
    for s in range(np_):
        cols = slice(s * LANE, (s + 1) * LANE)
        step = cz[last, s] + beta * s_c[s]
        along = r_c[s] + beta * d_c[s]
        sol_out[:, cols] = sol_c[s] + alpha * along
        res_out[:, cols] = r_c[s] - alpha * step
    hist_out[...] = hist[...].T[0:ITERS, :]
    for d in far_z:
        dz_copy(d).wait_send()


def on_device(np_, ngy, panels, diagonal, right, start):
    cases, cols = right.shape
    nslot = 2 * ngy
    per_chunk = nslot // 4
    span = LANE * per_chunk
    parts = nslot // per_chunk
    vm = lambda *shape: pltpu.VMEM(shape, F32)
    dma = lambda *shape: pltpu.SemaphoreType.DMA(shape)
    state = (np_, cases, LANE)
    wide = (nslot, cases, LANE)
    one = (cases, LANE)
    scratch = [
        vm(4, cols), vm(1, cols), vm(cases, cols), vm(cases, cols),
        vm(nslot, 4, LANE),
        pltpu.VMEM((parts, span, cols), BF16), pltpu.VMEM((parts, span, cols), BF16), pltpu.VMEM((48, cols), BF16), pltpu.VMEM((3 * cases, span), BF16),
        vm(*one), vm(3, *wide), vm(2, *state), vm(np_, *one), vm(2, np_, *one), vm(8, LANE), vm(2, np_, 8, LANE),
        vm(cases, cols),
        vm(*state), vm(*state), vm(*state), vm(*state), vm(*wide), vm(*wide),
        vm(*one), vm(*one), vm(*one), vm(*one), vm(*one), vm(3, *one),
        vm(8, LANE), vm(nslot, 8, LANE), vm(8, LANE), vm(np_, 8, LANE),
        dma(5), dma(nslot), dma(nslot), dma(nslot), dma(3, nslot), dma(np_), dma(2, np_), dma(np_), dma(2, np_), dma(np_), dma(2, np_),
        dma(nslot), dma(nslot), dma(np_), dma(np_),
    ]
    return pl.pallas_call(
        functools.partial(cg_kernel, np_, ngy, cases, per_chunk),
        out_shape=(
            jax.ShapeDtypeStruct((cases, cols), F32),
            jax.ShapeDtypeStruct((cases, cols), F32),
            jax.ShapeDtypeStruct((ITERS, cases), F32),
        ),
        in_specs=[pl.BlockSpec(memory_space=pltpu.HBM)] * 4,
        out_specs=tuple([pl.BlockSpec(memory_space=pltpu.VMEM)] * 3),
        scratch_shapes=scratch,
        compiler_params=pltpu.CompilerParams(
            collective_id=0, has_side_effects=True, vmem_limit_bytes=60 * 1024 * 1024
        ),
        name="cg",
    )(panels, diagonal[None, :], right, start)


def solution(mesh):
    cut = P(None, ("gy", "gz"))
    sizes = dict(mesh.shape)
    return jax.shard_map(
        functools.partial(on_device, sizes["gx"], sizes["gy"]),
        mesh=mesh,
        in_specs=(cut, P(("gy", "gz")), cut, cut),
        out_specs=(cut, cut, P()),
        check_vma=False,
    )
```

```python
import functools
import math
import jax
import jax.numpy as jnp
from jax import lax
from jax.experimental import pallas as pl
from jax.experimental.pallas import tpu as pltpu
from jax.sharding import PartitionSpec as P

ITERS = 4
SOFT_SQ = 0.0025
LANE = 128
MESH = pl.DeviceIdType.MESH
F32 = jnp.float32
BF16 = jnp.bfloat16


def ring_distance(step, size):
    return min(step, size - step)


def chip_offsets(side):
    every = [(dx, dy) for dx in range(side) for dy in range(side)]
    return sorted(every, key=lambda o: (ring_distance(o[0], side) + ring_distance(o[1], side), o))


def cg_kernel(np_, ngy, cases, per_chunk,
              panels_hbm, diagonal_hbm, right_hbm, start_hbm, sol_out, res_out, hist_out,
              panels, partner, diagonal, right, start, rowpan, ghi, glo, rhs, lhs_last, vp, vg, cz, px, px_in, ps, rs,
              dots_out, dots_in, acc, sol_c, r_c, s_c, d_c, r_r, s_r, zdir, gprev, aprev, hist, scal, sums,
              dtile, dplane, dsum, dz,
              in_s, pan_s, pan_r, pp_s, pp_r, ag_s, ag_r, z_s, z_r, px_s, px_r, rs_s, rs_r, dt_s, dt_r,
              dp_s, dp_r, dz_s, dz_r):
    side = math.isqrt(ngy)
    offsets = chip_offsets(side)
    order = list(range(ngy))
    place = {k: i for i, k in enumerate(order)}
    nslot = len(order)
    nchunk = nslot // per_chunk
    cols_all = np_ * LANE
    inv_root = (2 * nslot * np_ * LANE) ** -0.5
    p = lax.axis_index("gx")
    gy = lax.axis_index("gy")
    gz = lax.axis_index("gz")
    x, y = gy // side, lax.rem(gy, side)
    own = pl.ds(pl.multiple_of(p * LANE, LANE), LANE)
    lane = lax.broadcasted_iota(jnp.int32, (cases, LANE), 1)
    lane8 = lax.broadcasted_iota(jnp.int32, (8, LANE), 1)
    row8 = lax.broadcasted_iota(jnp.int32, (8, LANE), 0)
    groups = cases // 8
    far_z = sorted(range(1, np_), key=lambda d: -ring_distance(d, np_))
    every_chip = range(ngy)
    everyone = [(k, core) for k in range(ngy) for core in range(2) if k + core]

    def chip_at(k, sign):
        dx, dy = offsets[k]
        if sign < 0:
            dx, dy = (side - dx) % side, (side - dy) % side
        return lax.rem(x + dx, side) * side + lax.rem(y + dy, side)

    def chip(k, core):
        return (p, chip_at(k, -1), gz if core == 0 else 1 - gz)

    def z_of(d):
        return lax.rem(p + d, np_)

    def z_dev(d):
        return (z_of(d), gy, gz)

    def remote(src, dst, send, recv, dev):
        return pltpu.make_async_remote_copy(src, dst, send, recv, device_id=dev, device_id_type=MESH)

    def loop(lo, hi, fn):
        def step(i, carry):
            fn(i)
            return carry
        lax.fori_loop(lo, hi, step, 0)

    def plane_copy(k, core):
        i = 2 * k + core
        return remote(dtile, dplane.at[i], dp_s.at[i], dp_r.at[i], chip(k, core))

    def pan_copy(k):
        i = place[k]
        return remote(panels.at[:, own], rowpan.at[i], pan_s.at[i], pan_r.at[i], chip(k, 1))

    def partner_copy():
        return remote(panels, partner, pp_s, pp_r, chip(0, 1))

    def ag_copy(k, buf):
        i = place[k]
        return remote(vp, vg.at[buf, i], ag_s.at[i], ag_r.at[buf, i], chip(k, 1))

    def px_copy(par):
        return remote(px, px_in.at[par], px_s, px_r.at[par], chip(0, 1))

    def zg_send(d, par):
        return remote(vp, cz.at[par, p], z_s.at[d], z_r.at[par, p], z_dev(d))

    def zg_recv(d, par):
        o = z_of(d)
        return remote(vp, cz.at[par, o], z_s.at[d], z_r.at[par, o], z_dev(d))

    def rs_copy(d, par):
        return remote(ps.at[z_of(d)], rs.at[par, d], rs_s.at[d], rs_r.at[par, d], (z_of(d), gy, 1 - gz))

    def dt_copy(d, core, par):
        i = 2 * d + core
        return remote(dots_out, dots_in.at[par, i], dt_s.at[i], dt_r.at[par, i], (z_of(d), gy, gz if core == 0 else 1 - gz))

    dot_peers = [(d, core) for d in far_z + [0] for core in range(2) if d + core]

    def dz_copy(d):
        return remote(dsum, dz.at[d], dz_s.at[d], dz_r.at[d], (z_of(d), gy, 1 - gz))

    loads = [
        pltpu.make_async_copy(panels_hbm, panels, in_s.at[0]),
        pltpu.make_async_copy(start_hbm.at[:, own], vp, in_s.at[1]),
        pltpu.make_async_copy(start_hbm, start, in_s.at[2]),
        pltpu.make_async_copy(right_hbm, right, in_s.at[3]),
        pltpu.make_async_copy(diagonal_hbm, diagonal, in_s.at[4]),
    ]
    for load in loads:
        load.start()

    barrier = pltpu.get_barrier_semaphore()
    for k, core in reversed(everyone):
        pl.semaphore_signal(barrier, inc=1, device_id=chip(k, core), device_id_type=MESH)
    for d in far_z:
        for core in range(2):
            dev = (z_of(d), gy, gz if core == 0 else 1 - gz)
            pl.semaphore_signal(barrier, inc=1, device_id=dev, device_id_type=MESH)

    loads[0].wait()

    def split(value):
        top = value.astype(BF16).astype(F32)
        mid = (value - top).astype(BF16).astype(F32)
        return top, mid, value - top - mid

    def other_side(pan, base):
        for s in range(np_):
            here = slice(s * LANE, (s + 1) * LANE)
            ax, ay, at = (pan[i:i + 1, here] for i in range(3))
            other = jnp.where(row8 == 4, 1.0, jnp.where(row8 == 5, ax * ax + ay * ay + at * at, 0.0))
            for i, value in enumerate((ax, ay, at)):
                other = jnp.where(row8 == i, -2.0 * value, other)
            top, mid, low = split(other)
            there = slice(base + s * LANE, base + (s + 1) * LANE)
            rhs[:, there] = jnp.concatenate([top, mid, low, top, mid, top], 0).astype(BF16)

    other_side(panels, 0)

    for load in loads[1:]:
        load.wait()
    for s in range(np_):
        sol_c[s] = start[:, s * LANE:(s + 1) * LANE]
    sums[...] = jnp.zeros_like(sums)
    s_c[...] = jnp.zeros_like(s_c)
    d_c[...] = jnp.zeros_like(d_c)
    r_c[...] = jnp.zeros_like(r_c)
    s_r[...] = jnp.zeros_like(s_r)
    r_r[...] = jnp.zeros_like(r_r)
    zdir[...] = jnp.zeros_like(zdir)
    gprev[...] = jnp.ones_like(gprev)
    aprev[...] = jnp.ones_like(aprev)
    hist[...] = jnp.zeros_like(hist)

    with jax.named_scope("barrier"):
        pl.semaphore_wait(barrier, 2 * ngy - 1 + 2 * (np_ - 1))
    partner_copy().start()
    for k in reversed(every_chip):
        pan_copy(k).start()

    def send_piece(buf):
        for k in every_chip:
            ag_copy(k, buf).start()

    send_piece(0)
    partner_copy().wait_recv()
    other_side(partner, cols_all)

    def build(c):
        for n in range(per_chunk):
            i = c * per_chunk + n
            pan = rowpan[i]
            ax, ay, at = (pan[j:j + 1] for j in range(3))
            tile = jnp.where(row8 == 4, ax * ax + ay * ay + at * at + SOFT_SQ, jnp.where(row8 == 5, 1.0, 0.0))
            for j, value in enumerate((ax, ay, at)):
                tile = jnp.where(row8 == j, value, tile)
            top, mid, low = split(tile)
            lhs = jnp.concatenate([top, top, top, mid, mid, low], 0).T.astype(BF16)
            there = slice(n * LANE, (n + 1) * LANE)
            for t in range(2 * cols_all // width):
                cols = slice(t * width, (t + 1) * width)
                value = lax.rsqrt(jnp.dot(lhs, rhs[:, cols], preferred_element_type=F32))
                top = value.astype(BF16)
                ghi[c, there, cols] = top
                glo[c, there, cols] = (value - top.astype(F32)).astype(BF16)

    width = 2 * LANE

    def pack_dots(parts):
        out = jnp.zeros((8, LANE), F32)
        for d in range(3):
            for g in range(groups):
                out = jnp.where(lane8 == groups * d + g, parts[d][8 * g:8 * g + 8, :], out)
        return out

    def unpack_dots(got):
        out = []
        for d in range(3):
            out.append(jnp.concatenate([got[:, groups * d + g:groups * d + g + 1] for g in range(groups)], 0))
        return out

    def row_sum(value):
        return jnp.sum(value, axis=1, keepdims=True)

    def coefficients(got, turn):
        gamma, delta, omega = unpack_dots(got)
        hist[...] = jnp.where(lane == turn, jnp.sqrt(omega / gamma), hist[...])
        gamma_prev = gprev[:, 0:1]
        alpha_prev = aprev[:, 0:1]
        beta = jnp.where(turn == 0, 0.0, gamma / gamma_prev)
        alpha = gamma / (delta - beta * gamma / alpha_prev)
        gprev[...] = jnp.broadcast_to(gamma, (cases, LANE))
        aprev[...] = jnp.broadcast_to(alpha, (cases, LANE))
        scal[...] = jnp.broadcast_to(beta, (cases, LANE))
        return alpha, beta

    def rows_of(c, buf):
        pieces = []
        for i in range(c * per_chunk, (c + 1) * per_chunk):
            value = vg[buf, i] * (rowpan[i, 3:4, :] * inv_root)
            top = value.astype(BF16)
            value = value - top.astype(F32)
            mid = value.astype(BF16)
            low = (value - mid.astype(F32)).astype(BF16)
            pieces.append(jnp.concatenate([top, mid, low], 0))
        return jnp.concatenate(pieces, 1)

    def product(lhs, top, low):
        main = jnp.dot(lhs, top, preferred_element_type=F32)
        rest = jnp.dot(lhs[:2 * cases], low, preferred_element_type=F32)
        small = main[2 * cases:] + rest[cases:]
        return main[:cases] + (main[cases:2 * cases] + rest[:cases] + small)

    def matmul(c, buf):
        part = product(rows_of(c, buf), ghi[c], glo[c])
        acc[...] = part if c == 0 else part + acc[...]

    def last_product(side_of):
        c = nchunk - 1
        cols = slice(side_of * cols_all, (side_of + 1) * cols_all)
        return acc[:, cols] + product(lhs_last[...], ghi[c, :, cols], glo[c, :, cols])

    def dots(first, stop, buf, parts):
        g, d, o = parts
        for i in range(first, stop):
            r, a = r_r[i], vg[buf, i]
            g, d, o = g + r * r, d + a * r, o + a * a
        return g, d, o

    def arrive(c, buf):
        with jax.named_scope(f"ag_wait{c}"):
            for k in order[c * per_chunk:(c + 1) * per_chunk]:
                ag_copy(k, buf).wait_recv()

    with jax.named_scope("build"):
        for c in range(nchunk):
            with jax.named_scope(f"pan_wait{c}"):
                for k in order[c * per_chunk:(c + 1) * per_chunk]:
                    pan_copy(k).wait_recv()
            if c > 0:
                arrive(c - 1, 0)
            build(c)
            if c > 0:
                matmul(c - 1, 0)
    partner_copy().wait_send()
    for k in every_chip:
        pan_copy(k).wait_send()

    def event(e, carry):
        par = lax.rem(e, 2)
        nxt = 1 - par
        buf = lax.rem(e, 3)
        after = lax.rem(e + 1, 3)
        @pl.when(e > 0)
        def _():
            for c in range(nchunk - 1):
                arrive(c, buf)
                with jax.named_scope(f"matmul{c}"):
                    matmul(c, buf)
                    parts = (sums[0], sums[1], sums[2])
                    if c == 0:
                        parts = (jnp.zeros((cases, LANE), F32),) * 3
                    sums[0], sums[1], sums[2] = dots(c * per_chunk, (c + 1) * per_chunk, buf, parts)
        arrive(nchunk - 1, buf)
        with jax.named_scope("last_A"):
            lhs_last[...] = rows_of(nchunk - 1, buf)
            part = last_product(0)
            for s in range(np_):
                px[s] = part[:, s * LANE:(s + 1) * LANE]
            parts = dots((nchunk - 1) * per_chunk, nslot, buf, (sums[0], sums[1], sums[2]))
            dots_out[...] = pack_dots([row_sum(v) for v in parts])
        px_copy(par).start()

        @pl.when(e >= 2)
        def _():
            for d, core in dot_peers:
                dt_copy(d, core, par).start()
        with jax.named_scope("last_B"):
            part = last_product(1)
            for s in range(np_):
                ps[s] = part[:, s * LANE:(s + 1) * LANE]
        dots_in[par, 0] = dots_out[...]
        with jax.named_scope("px_wait"):
            px_copy(par).wait_recv()
        for d in far_z + [0]:
            to = z_of(d)
            ps[to] = ps[to] + px_in[par, to]
            rs_copy(d, par).start()
        px_copy(par).wait_send()
        for k in every_chip:
            ag_copy(k, buf).wait_send()

        @pl.when(e > 0)
        def _():
            for d in far_z:
                zg_send(d, par).wait_send()
            cz[par, p] = vp[...]
        with jax.named_scope("rs_wait"):
            @pl.when(e >= 2)
            def _():
                for d, core in dot_peers:
                    dt_copy(d, core, par).wait_recv()
            for d in far_z + [0]:
                rs_copy(d, par).wait_recv()
        got = jnp.sum(rs[par], axis=0)
        fresh = got * panels[3:4, own] + diagonal[0:1, own] * vp[...]

        @pl.when(e == 0)
        def _():
            vp[...] = right[:, own] - fresh

        @pl.when(e == 1)
        def _():
            vp[...] = fresh

        @pl.when(e >= 2)
        def _():
            alpha, beta = coefficients(jnp.sum(dots_in[par], axis=0), e - 2)
            z = fresh + beta * zdir[...]
            zdir[...] = z
            vp[...] = vp[...] - alpha * z

        @pl.when(e < ITERS)
        def _():
            send_piece(after)
        for d in far_z:
            zg_send(d, nxt).start()
        with jax.named_scope("rs_send"):
            for d in far_z + [0]:
                rs_copy(d, par).wait_send()

        @pl.when(e >= 2)
        def _():
            for d, core in dot_peers:
                dt_copy(d, core, par).wait_send()

        @pl.when(e > 0)
        def _():
            for d in far_z:
                zg_recv(d, par).wait_recv()

        @pl.when(e == 1)
        def _():
            loop(0, nslot, lambda s: r_r.__setitem__(s, vg[buf, s]))
            loop(0, np_, lambda s: r_c.__setitem__(s, cz[par, s]))

        @pl.when(e >= 2)
        def _():
            alpha = aprev[...]
            beta = scal[...]

            def rows(s):
                step = vg[buf, s] + beta * s_r[s]
                s_r[s] = step
                r_r[s] = r_r[s] - alpha * step
            loop(0, nslot, rows)

            def cols(s):
                step = cz[par, s] + beta * s_c[s]
                s_c[s] = step
                along = r_c[s] + beta * d_c[s]
                d_c[s] = along
                sol_c[s] = sol_c[s] + alpha * along
                r_c[s] = r_c[s] - alpha * step
            loop(0, np_, cols)
        return carry

    lax.fori_loop(0, ITERS + 1, event, 0)

    last = (ITERS + 1) % 2
    r = r_c[p]
    a = vp[...]
    dtile[...] = pack_dots([row_sum(r * r), row_sum(a * r), row_sum(a * a)])
    for k, core in reversed(everyone):
        plane_copy(k, core).start()
    dplane[0] = dtile[...]
    cz[last, p] = vp[...]
    with jax.named_scope("dp_wait"):
        for k, core in everyone:
            plane_copy(k, core).wait_recv()
    dsum[...] = jnp.sum(dplane[...], axis=0)
    for d in far_z:
        dz_copy(d).start()
    dz[0] = dsum[...]
    for k, core in everyone:
        plane_copy(k, core).wait_send()
    for d in far_z:
        zg_send(d, last).wait_send()
    with jax.named_scope("dz_wait"):
        for d in far_z:
            zg_recv(d, last).wait_recv()
        for d in far_z:
            dz_copy(d).wait_recv()
    alpha, beta = coefficients(jnp.sum(dz[...], axis=0), ITERS - 1)
    for s in range(np_):
        cols = slice(s * LANE, (s + 1) * LANE)
        step = cz[last, s] + beta * s_c[s]
        along = r_c[s] + beta * d_c[s]
        sol_out[:, cols] = sol_c[s] + alpha * along
        res_out[:, cols] = r_c[s] - alpha * step
    hist_out[...] = hist[...].T[0:ITERS, :]
    for d in far_z:
        dz_copy(d).wait_send()


def hand_over(*refs):
    n = (len(refs) - 1) // 3
    src, dst, mid, sems = refs[:n], refs[n:2 * n], refs[2 * n:3 * n], refs[3 * n]
    loads = [pltpu.make_async_copy(src[i], mid[i], sems.at[0, i]) for i in range(n)]
    stores = [pltpu.make_async_copy(mid[i], dst[i], sems.at[1, i]) for i in range(n)]
    for load in loads:
        load.start()
    for load, store in zip(loads, stores):
        load.wait()
        store.start()
    for store in stores:
        store.wait()


def on_device(np_, ngy, panels, diagonal, right, start):
    cases, cols = right.shape
    nslot = ngy
    per_chunk = nslot // 4
    span = LANE * per_chunk
    parts = nslot // per_chunk
    vm = lambda *shape: pltpu.VMEM(shape, F32)
    half = lambda *shape: pltpu.VMEM(shape, BF16)
    dma = lambda *shape: pltpu.SemaphoreType.DMA(shape)
    state = (np_, cases, LANE)
    wide = (nslot, cases, LANE)
    one = (cases, LANE)
    scratch = [
        vm(4, cols), vm(4, cols), vm(1, cols), vm(cases, cols), vm(cases, cols), vm(nslot, 4, LANE),
        half(parts, span, 2 * cols), half(parts, span, 2 * cols), half(48, 2 * cols), half(3 * cases, span),
        vm(*one), vm(3, *wide), vm(2, *state), vm(*state), vm(2, *state), vm(*state), vm(2, *state),
        vm(8, LANE), vm(2, 2 * np_, 8, LANE), vm(cases, 2 * cols),
        vm(*state), vm(*state), vm(*state), vm(*state), vm(*wide), vm(*wide),
        vm(*one), vm(*one), vm(*one), vm(*one), vm(*one), vm(3, *one),
        vm(8, LANE), vm(2 * nslot, 8, LANE), vm(8, LANE), vm(np_, 8, LANE),
        dma(5), dma(nslot), dma(nslot), pltpu.SemaphoreType.DMA, pltpu.SemaphoreType.DMA,
        dma(nslot), dma(3, nslot), dma(np_), dma(2, np_), pltpu.SemaphoreType.DMA, dma(2),
        dma(np_), dma(2, np_), dma(2 * np_), dma(2, 2 * np_),
        dma(2 * nslot), dma(2 * nslot), dma(np_), dma(np_),
    ]
    results = pl.pallas_call(
        functools.partial(cg_kernel, np_, ngy, cases, per_chunk),
        out_shape=(
            jax.ShapeDtypeStruct((cases, cols), F32),
            jax.ShapeDtypeStruct((cases, cols), F32),
            jax.ShapeDtypeStruct((ITERS, cases), F32),
        ),
        in_specs=[pl.BlockSpec(memory_space=pltpu.HBM)] * 4,
        out_specs=tuple([pl.BlockSpec(memory_space=pltpu.VMEM)] * 3),
        scratch_shapes=scratch,
        compiler_params=pltpu.CompilerParams(
            collective_id=0, has_side_effects=True, vmem_limit_bytes=60 * 1024 * 1024
        ),
        name="cg",
    )(panels, diagonal[None, :], right, start)
    return pl.pallas_call(
        hand_over,
        out_shape=tuple(jax.ShapeDtypeStruct(r.shape, r.dtype) for r in results),
        in_specs=[pl.BlockSpec(memory_space=pltpu.HBM)] * 3,
        out_specs=tuple([pl.BlockSpec(memory_space=pltpu.HBM)] * 3),
        scratch_shapes=[pltpu.VMEM(r.shape, r.dtype) for r in results] + [pltpu.SemaphoreType.DMA((2, 3))],
        compiler_params=pltpu.CompilerParams(vmem_limit_bytes=60 * 1024 * 1024),
        name="hand_over",
    )(*results)


def solution(mesh):
    cut = P(None, ("gy", "gz"))
    sizes = dict(mesh.shape)
    return jax.shard_map(
        functools.partial(on_device, sizes["gx"], sizes["gy"]),
        mesh=mesh,
        in_specs=(cut, P(("gy", "gz")), cut, cut),
        out_specs=(cut, cut, P()),
        check_vma=False,
    )
```

```python
import functools
import math
import jax
import jax.numpy as jnp
from jax import lax
from jax.experimental import pallas as pl
from jax.experimental.pallas import tpu as pltpu
from jax.sharding import PartitionSpec as P

ITERS = 4
SOFT_SQ = 0.0025
LANE = 128
MESH = pl.DeviceIdType.MESH
F32 = jnp.float32
BF16 = jnp.bfloat16


def ring_distance(step, size):
    return min(step, size - step)


def chip_offsets(side):
    every = [(dx, dy) for dx in range(side) for dy in range(side)]
    return sorted(every, key=lambda o: (ring_distance(o[0], side) + ring_distance(o[1], side), o))


def chunk_bounds(nslot):
    step = nslot // 4
    short = step // 4
    return [0, step + short, 2 * step + 2 * short, 3 * step + 2 * short, nslot]


def cg_kernel(np_, ngy, cases,
              panels_hbm, diagonal_hbm, right_hbm, start_hbm, sol_out, res_out, hist_out,
              panels, partner, diagonal, right, start, rowpan, ghi, glo, rhs, lhs_last, vp, vg, cz, px, px_in, ps, rs,
              dots_out, dots_in, acc, sol_c, r_c, s_c, d_c, r_r, s_r, zdir, gprev, aprev, hist, scal, sums,
              dtile, dplane, dsum, dz,
              in_s, pan_s, pan_r, pp_s, pp_r, ag_s, ag_r, z_s, z_r, px_s, px_r, rs_s, rs_r, dt_s, dt_r,
              dp_s, dp_r, dz_s, dz_r):
    side = math.isqrt(ngy)
    offsets = chip_offsets(side)
    order = list(range(ngy))
    place = {k: i for i, k in enumerate(order)}
    nslot = len(order)
    bounds = chunk_bounds(nslot)
    nchunk = len(bounds) - 1
    cols_all = np_ * LANE
    inv_root = (2 * nslot * np_ * LANE) ** -0.5
    p = lax.axis_index("gx")
    gy = lax.axis_index("gy")
    gz = lax.axis_index("gz")
    x, y = gy // side, lax.rem(gy, side)
    own = pl.ds(pl.multiple_of(p * LANE, LANE), LANE)
    lane = lax.broadcasted_iota(jnp.int32, (cases, LANE), 1)
    lane8 = lax.broadcasted_iota(jnp.int32, (8, LANE), 1)
    row8 = lax.broadcasted_iota(jnp.int32, (8, LANE), 0)
    groups = cases // 8
    far_z = sorted(range(1, np_), key=lambda d: -ring_distance(d, np_))
    every_chip = range(ngy)
    everyone = [(k, core) for k in range(ngy) for core in range(2) if k + core]

    def chip_at(k, sign):
        dx, dy = offsets[k]
        if sign < 0:
            dx, dy = (side - dx) % side, (side - dy) % side
        return lax.rem(x + dx, side) * side + lax.rem(y + dy, side)

    def chip(k, core):
        return (p, chip_at(k, -1), gz if core == 0 else 1 - gz)

    def z_of(d):
        return lax.rem(p + d, np_)

    def z_dev(d):
        return (z_of(d), gy, gz)

    def remote(src, dst, send, recv, dev):
        return pltpu.make_async_remote_copy(src, dst, send, recv, device_id=dev, device_id_type=MESH)

    def loop(lo, hi, fn):
        def step(i, carry):
            fn(i)
            return carry
        lax.fori_loop(lo, hi, step, 0)

    def plane_copy(k, core):
        i = 2 * k + core
        return remote(dtile, dplane.at[i], dp_s.at[i], dp_r.at[i], chip(k, core))

    def pan_copy(k):
        i = place[k]
        return remote(panels.at[:, own], rowpan.at[i], pan_s.at[i], pan_r.at[i], chip(k, 1))

    def partner_copy():
        return remote(panels, partner, pp_s, pp_r, chip(0, 1))

    def ag_copy(k, buf):
        i = place[k]
        return remote(vp, vg.at[buf, i], ag_s.at[i], ag_r.at[buf, i], chip(k, 1))

    def px_copy(par):
        return remote(px, px_in.at[par], px_s, px_r.at[par], chip(0, 1))

    def zg_send(d, par):
        return remote(vp, cz.at[par, p], z_s.at[d], z_r.at[par, p], z_dev(d))

    def zg_recv(d, par):
        o = z_of(d)
        return remote(vp, cz.at[par, o], z_s.at[d], z_r.at[par, o], z_dev(d))

    def rs_copy(d, par):
        return remote(ps.at[z_of(d)], rs.at[par, d], rs_s.at[d], rs_r.at[par, d], (z_of(d), gy, 1 - gz))

    def dt_copy(d, core, par):
        i = 2 * d + core
        return remote(dots_out, dots_in.at[par, i], dt_s.at[i], dt_r.at[par, i], (z_of(d), gy, gz if core == 0 else 1 - gz))

    dot_peers = [(d, core) for d in far_z + [0] for core in range(2) if d + core]

    def dz_copy(d):
        return remote(dsum, dz.at[d], dz_s.at[d], dz_r.at[d], (z_of(d), gy, 1 - gz))

    loads = [
        pltpu.make_async_copy(panels_hbm, panels, in_s.at[0]),
        pltpu.make_async_copy(start_hbm.at[:, own], vp, in_s.at[1]),
        pltpu.make_async_copy(start_hbm, start, in_s.at[2]),
        pltpu.make_async_copy(right_hbm, right, in_s.at[3]),
        pltpu.make_async_copy(diagonal_hbm, diagonal, in_s.at[4]),
    ]
    for load in loads:
        load.start()

    barrier = pltpu.get_barrier_semaphore()
    for k, core in reversed(everyone):
        pl.semaphore_signal(barrier, inc=1, device_id=chip(k, core), device_id_type=MESH)
    for d in far_z:
        for core in range(2):
            dev = (z_of(d), gy, gz if core == 0 else 1 - gz)
            pl.semaphore_signal(barrier, inc=1, device_id=dev, device_id_type=MESH)

    loads[0].wait()

    def split(value):
        top = value.astype(BF16).astype(F32)
        mid = (value - top).astype(BF16).astype(F32)
        return top, mid, value - top - mid

    def other_side(pan, base):
        for s in range(np_):
            here = slice(s * LANE, (s + 1) * LANE)
            ax, ay, at = (pan[i:i + 1, here] for i in range(3))
            other = jnp.where(row8 == 4, 1.0, jnp.where(row8 == 5, ax * ax + ay * ay + at * at, 0.0))
            for i, value in enumerate((ax, ay, at)):
                other = jnp.where(row8 == i, -2.0 * value, other)
            top, mid, low = split(other)
            there = slice(base + s * LANE, base + (s + 1) * LANE)
            rhs[:, there] = jnp.concatenate([top, mid, low, top, mid, top], 0).astype(BF16)

    other_side(panels, 0)

    for load in loads[1:]:
        load.wait()
    for s in range(np_):
        sol_c[s] = start[:, s * LANE:(s + 1) * LANE]
    sums[...] = jnp.zeros_like(sums)
    s_c[...] = jnp.zeros_like(s_c)
    d_c[...] = jnp.zeros_like(d_c)
    r_c[...] = jnp.zeros_like(r_c)
    s_r[...] = jnp.zeros_like(s_r)
    r_r[...] = jnp.zeros_like(r_r)
    zdir[...] = jnp.zeros_like(zdir)
    gprev[...] = jnp.ones_like(gprev)
    aprev[...] = jnp.ones_like(aprev)
    hist[...] = jnp.zeros_like(hist)

    with jax.named_scope("barrier"):
        pl.semaphore_wait(barrier, 2 * ngy - 1 + 2 * (np_ - 1))
    partner_copy().start()
    for k in reversed(every_chip):
        pan_copy(k).start()

    def send_piece(buf):
        for k in every_chip:
            ag_copy(k, buf).start()

    send_piece(0)
    partner_copy().wait_recv()
    other_side(partner, cols_all)

    def build(c):
        for i in range(bounds[c], bounds[c + 1]):
            pan = rowpan[i]
            ax, ay, at = (pan[j:j + 1] for j in range(3))
            tile = jnp.where(row8 == 4, ax * ax + ay * ay + at * at + SOFT_SQ, jnp.where(row8 == 5, 1.0, 0.0))
            for j, value in enumerate((ax, ay, at)):
                tile = jnp.where(row8 == j, value, tile)
            top, mid, low = split(tile)
            lhs = jnp.concatenate([top, top, top, mid, mid, low], 0).T.astype(BF16)
            there = slice(i * LANE, (i + 1) * LANE)
            for t in range(2 * cols_all // width):
                cols = slice(t * width, (t + 1) * width)
                value = lax.rsqrt(jnp.dot(lhs, rhs[:, cols], preferred_element_type=F32))
                top = value.astype(BF16)
                ghi[there, cols] = top
                glo[there, cols] = (value - top.astype(F32)).astype(BF16)

    width = 2 * LANE

    def pack_dots(parts):
        out = jnp.zeros((8, LANE), F32)
        for d in range(3):
            for g in range(groups):
                out = jnp.where(lane8 == groups * d + g, parts[d][8 * g:8 * g + 8, :], out)
        return out

    def unpack_dots(got):
        out = []
        for d in range(3):
            out.append(jnp.concatenate([got[:, groups * d + g:groups * d + g + 1] for g in range(groups)], 0))
        return out

    def row_sum(value):
        return jnp.sum(value, axis=1, keepdims=True)

    def coefficients(got, turn):
        gamma, delta, omega = unpack_dots(got)
        hist[...] = jnp.where(lane == turn, jnp.sqrt(omega / gamma), hist[...])
        gamma_prev = gprev[:, 0:1]
        alpha_prev = aprev[:, 0:1]
        beta = jnp.where(turn == 0, 0.0, gamma / gamma_prev)
        alpha = gamma / (delta - beta * gamma / alpha_prev)
        gprev[...] = jnp.broadcast_to(gamma, (cases, LANE))
        aprev[...] = jnp.broadcast_to(alpha, (cases, LANE))
        scal[...] = jnp.broadcast_to(beta, (cases, LANE))
        return alpha, beta

    def rows_of(c, buf):
        pieces = []
        for i in range(bounds[c], bounds[c + 1]):
            value = vg[buf, i] * (rowpan[i, 3:4, :] * inv_root)
            top = value.astype(BF16)
            value = value - top.astype(F32)
            mid = value.astype(BF16)
            low = (value - mid.astype(F32)).astype(BF16)
            pieces.append(jnp.concatenate([top, mid, low], 0))
        return jnp.concatenate(pieces, 1)

    def product(lhs, top, low):
        main = jnp.dot(lhs, top, preferred_element_type=F32)
        rest = jnp.dot(lhs[:2 * cases], low, preferred_element_type=F32)
        small = main[2 * cases:] + rest[cases:]
        return main[:cases] + (main[cases:2 * cases] + rest[:cases] + small)

    def matmul(c, buf):
        rows = slice(bounds[c] * LANE, bounds[c + 1] * LANE)
        part = product(rows_of(c, buf), ghi[rows], glo[rows])
        acc[...] = part if c == 0 else part + acc[...]

    def last_product(side_of):
        rows = slice(bounds[nchunk - 1] * LANE, nslot * LANE)
        cols = slice(side_of * cols_all, (side_of + 1) * cols_all)
        return acc[:, cols] + product(lhs_last[...], ghi[rows, cols], glo[rows, cols])

    def dots(first, stop, buf, parts):
        g, d, o = parts
        for i in range(first, stop):
            r, a = r_r[i], vg[buf, i]
            g, d, o = g + r * r, d + a * r, o + a * a
        return g, d, o

    def arrive(c, buf):
        with jax.named_scope(f"ag_wait{c}"):
            for k in order[bounds[c]:bounds[c + 1]]:
                ag_copy(k, buf).wait_recv()

    with jax.named_scope("build"):
        for c in range(nchunk):
            with jax.named_scope(f"pan_wait{c}"):
                for k in order[bounds[c]:bounds[c + 1]]:
                    pan_copy(k).wait_recv()
            if c > 0:
                arrive(c - 1, 0)
            build(c)
            if c > 0:
                matmul(c - 1, 0)
    partner_copy().wait_send()
    for k in every_chip:
        pan_copy(k).wait_send()

    def event(e, carry):
        par = lax.rem(e, 2)
        nxt = 1 - par
        buf = lax.rem(e, 3)
        after = lax.rem(e + 1, 3)
        @pl.when(e > 0)
        def _():
            for c in range(nchunk - 1):
                arrive(c, buf)
                with jax.named_scope(f"matmul{c}"):
                    matmul(c, buf)
                    parts = (sums[0], sums[1], sums[2])
                    if c == 0:
                        parts = (jnp.zeros((cases, LANE), F32),) * 3
                    sums[0], sums[1], sums[2] = dots(bounds[c], bounds[c + 1], buf, parts)
        arrive(nchunk - 1, buf)
        with jax.named_scope("last_A"):
            lhs_last[...] = rows_of(nchunk - 1, buf)
            part = last_product(0)
            for s in range(np_):
                px[s] = part[:, s * LANE:(s + 1) * LANE]
            parts = dots(bounds[nchunk - 1], nslot, buf, (sums[0], sums[1], sums[2]))
            dots_out[...] = pack_dots([row_sum(v) for v in parts])
        px_copy(par).start()

        @pl.when(e >= 2)
        def _():
            for d, core in dot_peers:
                dt_copy(d, core, par).start()
        with jax.named_scope("last_B"):
            part = last_product(1)
            for s in range(np_):
                ps[s] = part[:, s * LANE:(s + 1) * LANE]
        dots_in[par, 0] = dots_out[...]
        with jax.named_scope("px_wait"):
            px_copy(par).wait_recv()
        for d in far_z + [0]:
            to = z_of(d)
            ps[to] = ps[to] + px_in[par, to]
            rs_copy(d, par).start()
        px_copy(par).wait_send()
        for k in every_chip:
            ag_copy(k, buf).wait_send()

        @pl.when(e > 0)
        def _():
            for d in far_z:
                zg_send(d, par).wait_send()
            cz[par, p] = vp[...]
        with jax.named_scope("rs_wait"):
            @pl.when(e >= 2)
            def _():
                for d, core in dot_peers:
                    dt_copy(d, core, par).wait_recv()
                coefficients(jnp.sum(dots_in[par], axis=0), e - 2)
            for d in far_z + [0]:
                rs_copy(d, par).wait_recv()
        got = jnp.sum(rs[par], axis=0)
        fresh = got * panels[3:4, own] + diagonal[0:1, own] * vp[...]

        @pl.when(e == 0)
        def _():
            vp[...] = right[:, own] - fresh

        @pl.when(e == 1)
        def _():
            vp[...] = fresh

        @pl.when(e >= 2)
        def _():
            z = fresh + scal[...] * zdir[...]
            zdir[...] = z
            vp[...] = vp[...] - aprev[...] * z

        @pl.when(e < ITERS)
        def _():
            send_piece(after)
        for d in far_z:
            zg_send(d, nxt).start()
        with jax.named_scope("rs_send"):
            for d in far_z + [0]:
                rs_copy(d, par).wait_send()

        @pl.when(e >= 2)
        def _():
            for d, core in dot_peers:
                dt_copy(d, core, par).wait_send()

        @pl.when(e > 0)
        def _():
            for d in far_z:
                zg_recv(d, par).wait_recv()

        @pl.when(e == 1)
        def _():
            loop(0, nslot, lambda s: r_r.__setitem__(s, vg[buf, s]))
            loop(0, np_, lambda s: r_c.__setitem__(s, cz[par, s]))

        @pl.when(e >= 2)
        def _():
            alpha = aprev[...]
            beta = scal[...]

            def rows(s):
                step = vg[buf, s] + beta * s_r[s]
                s_r[s] = step
                r_r[s] = r_r[s] - alpha * step
            loop(0, jnp.where(e < ITERS, nslot, 0), rows)

            def cols(s):
                step = cz[par, s] + beta * s_c[s]
                s_c[s] = step
                along = r_c[s] + beta * d_c[s]
                d_c[s] = along
                sol_c[s] = sol_c[s] + alpha * along
                r_c[s] = r_c[s] - alpha * step
            loop(0, np_, cols)
        return carry

    lax.fori_loop(0, ITERS + 1, event, 0)

    last = (ITERS + 1) % 2
    r = r_c[p]
    a = vp[...]
    dtile[...] = pack_dots([row_sum(r * r), row_sum(a * r), row_sum(a * a)])
    for k, core in reversed(everyone):
        plane_copy(k, core).start()
    dplane[0] = dtile[...]
    cz[last, p] = vp[...]
    with jax.named_scope("dp_wait"):
        for k, core in everyone:
            plane_copy(k, core).wait_recv()
    dsum[...] = jnp.sum(dplane[...], axis=0)
    for d in far_z:
        dz_copy(d).start()
    dz[0] = dsum[...]
    for k, core in everyone:
        plane_copy(k, core).wait_send()
    for d in far_z:
        zg_send(d, last).wait_send()
    with jax.named_scope("dz_wait"):
        for d in far_z:
            zg_recv(d, last).wait_recv()
        for d in far_z:
            dz_copy(d).wait_recv()
    alpha, beta = coefficients(jnp.sum(dz[...], axis=0), ITERS - 1)
    for s in range(np_):
        cols = slice(s * LANE, (s + 1) * LANE)
        step = cz[last, s] + beta * s_c[s]
        along = r_c[s] + beta * d_c[s]
        sol_out[:, cols] = sol_c[s] + alpha * along
        res_out[:, cols] = r_c[s] - alpha * step
    hist_out[...] = hist[...].T[0:ITERS, :]
    for d in far_z:
        dz_copy(d).wait_send()


def hand_over(*refs):
    n = (len(refs) - 1) // 3
    src, dst, mid, sems = refs[:n], refs[n:2 * n], refs[2 * n:3 * n], refs[3 * n]
    loads = [pltpu.make_async_copy(src[i], mid[i], sems.at[0, i]) for i in range(n)]
    stores = [pltpu.make_async_copy(mid[i], dst[i], sems.at[1, i]) for i in range(n)]
    for load in loads:
        load.start()
    for load, store in zip(loads, stores):
        load.wait()
        store.start()
    for store in stores:
        store.wait()


def on_device(np_, ngy, panels, diagonal, right, start):
    cases, cols = right.shape
    nslot = ngy
    bounds = chunk_bounds(nslot)
    span = LANE * (nslot - bounds[-2])
    vm = lambda *shape: pltpu.VMEM(shape, F32)
    half = lambda *shape: pltpu.VMEM(shape, BF16)
    dma = lambda *shape: pltpu.SemaphoreType.DMA(shape)
    state = (np_, cases, LANE)
    wide = (nslot, cases, LANE)
    one = (cases, LANE)
    scratch = [
        vm(4, cols), vm(4, cols), vm(1, cols), vm(cases, cols), vm(cases, cols), vm(nslot, 4, LANE),
        half(nslot * LANE, 2 * cols), half(nslot * LANE, 2 * cols), half(48, 2 * cols), half(3 * cases, span),
        vm(*one), vm(3, *wide), vm(2, *state), vm(*state), vm(2, *state), vm(*state), vm(2, *state),
        vm(8, LANE), vm(2, 2 * np_, 8, LANE), vm(cases, 2 * cols),
        vm(*state), vm(*state), vm(*state), vm(*state), vm(*wide), vm(*wide),
        vm(*one), vm(*one), vm(*one), vm(*one), vm(*one), vm(3, *one),
        vm(8, LANE), vm(2 * nslot, 8, LANE), vm(8, LANE), vm(np_, 8, LANE),
        dma(5), dma(nslot), dma(nslot), pltpu.SemaphoreType.DMA, pltpu.SemaphoreType.DMA,
        dma(nslot), dma(3, nslot), dma(np_), dma(2, np_), pltpu.SemaphoreType.DMA, dma(2),
        dma(np_), dma(2, np_), dma(2 * np_), dma(2, 2 * np_),
        dma(2 * nslot), dma(2 * nslot), dma(np_), dma(np_),
    ]
    results = pl.pallas_call(
        functools.partial(cg_kernel, np_, ngy, cases),
        out_shape=(
            jax.ShapeDtypeStruct((cases, cols), F32),
            jax.ShapeDtypeStruct((cases, cols), F32),
            jax.ShapeDtypeStruct((ITERS, cases), F32),
        ),
        in_specs=[pl.BlockSpec(memory_space=pltpu.HBM)] * 4,
        out_specs=tuple([pl.BlockSpec(memory_space=pltpu.VMEM)] * 3),
        scratch_shapes=scratch,
        compiler_params=pltpu.CompilerParams(
            collective_id=0, has_side_effects=True, vmem_limit_bytes=60 * 1024 * 1024
        ),
        name="cg",
    )(panels, diagonal[None, :], right, start)
    return pl.pallas_call(
        hand_over,
        out_shape=tuple(jax.ShapeDtypeStruct(r.shape, r.dtype) for r in results),
        in_specs=[pl.BlockSpec(memory_space=pltpu.HBM)] * 3,
        out_specs=tuple([pl.BlockSpec(memory_space=pltpu.HBM)] * 3),
        scratch_shapes=[pltpu.VMEM(r.shape, r.dtype) for r in results] + [pltpu.SemaphoreType.DMA((2, 3))],
        compiler_params=pltpu.CompilerParams(vmem_limit_bytes=60 * 1024 * 1024),
        name="hand_over",
    )(*results)


def solution(mesh):
    cut = P(None, ("gy", "gz"))
    sizes = dict(mesh.shape)
    return jax.shard_map(
        functools.partial(on_device, sizes["gx"], sizes["gy"]),
        mesh=mesh,
        in_specs=(cut, P(("gy", "gz")), cut, cut),
        out_specs=(cut, cut, P()),
        check_vma=False,
    )
```

```python
import functools
import math
import jax
import jax.numpy as jnp
from jax import lax
from jax.experimental import pallas as pl
from jax.experimental.pallas import tpu as pltpu
from jax.sharding import PartitionSpec as P

ITERS = 4
SOFT_SQ = 0.0025
LANE = 128
MESH = pl.DeviceIdType.MESH
F32 = jnp.float32
BF16 = jnp.bfloat16


def ring_distance(step, size):
    return min(step, size - step)


def chip_offsets(side):
    every = [(dx, dy) for dx in range(side) for dy in range(side)]
    return sorted(every, key=lambda o: (ring_distance(o[0], side) + ring_distance(o[1], side), o))


def chunk_bounds(nslot):
    step = nslot // 4
    short = step // 4
    return [0, step + short, 2 * step + 2 * short, 3 * step + 2 * short, nslot]


def cg_kernel(np_, ngy, cases,
              panels_hbm, diagonal_hbm, right_hbm, start_hbm, sol_out, res_out, hist_out,
              panels, partner, diagonal, right, start, rowpan, ghi, glo, rhs, lhs_last, vp, vg, cz, px, px_in, ps, rs,
              dots_out, dots_in, acc, sol_c, r_c, s_c, d_c, r_r, s_r, zdir, gprev, aprev, hist, scal, sums,
              dtile, dplane, dsum, dz,
              in_s, pan_s, pan_r, pp_s, pp_r, ag_s, ag_r, z_s, z_r, px_s, px_r, rs_s, rs_r, dt_s, dt_r,
              dp_s, dp_r, dz_s, dz_r):
    side = math.isqrt(ngy)
    offsets = chip_offsets(side)
    order = list(range(ngy))
    place = {k: i for i, k in enumerate(order)}
    nslot = len(order)
    bounds = chunk_bounds(nslot)
    nchunk = len(bounds) - 1
    cols_all = np_ * LANE
    inv_root = (2 * nslot * np_ * LANE) ** -0.5
    p = lax.axis_index("gx")
    gy = lax.axis_index("gy")
    gz = lax.axis_index("gz")
    x, y = gy // side, lax.rem(gy, side)
    own = pl.ds(pl.multiple_of(p * LANE, LANE), LANE)
    lane = lax.broadcasted_iota(jnp.int32, (cases, LANE), 1)
    lane8 = lax.broadcasted_iota(jnp.int32, (8, LANE), 1)
    row8 = lax.broadcasted_iota(jnp.int32, (8, LANE), 0)
    groups = cases // 8
    far_z = sorted(range(1, np_), key=lambda d: -ring_distance(d, np_))
    every_chip = range(ngy)
    everyone = [(k, core) for k in range(ngy) for core in range(2) if k + core]

    def chip_at(k, sign):
        dx, dy = offsets[k]
        if sign < 0:
            dx, dy = (side - dx) % side, (side - dy) % side
        return lax.rem(x + dx, side) * side + lax.rem(y + dy, side)

    def chip(k, core):
        return (p, chip_at(k, -1), gz if core == 0 else 1 - gz)

    def z_of(d):
        return lax.rem(p + d, np_)

    def z_dev(d):
        return (z_of(d), gy, gz)

    def remote(src, dst, send, recv, dev):
        return pltpu.make_async_remote_copy(src, dst, send, recv, device_id=dev, device_id_type=MESH)

    def loop(lo, hi, fn):
        def step(i, carry):
            fn(i)
            return carry
        lax.fori_loop(lo, hi, step, 0)

    def plane_copy(k, core):
        i = 2 * k + core
        return remote(dtile, dplane.at[i], dp_s.at[i], dp_r.at[i], chip(k, core))

    def pan_copy(k):
        i = place[k]
        return remote(panels.at[:, own], rowpan.at[i], pan_s.at[i], pan_r.at[i], chip(k, 1))

    def partner_copy():
        return remote(panels, partner, pp_s, pp_r, chip(0, 1))

    def ag_copy(k, buf):
        i = place[k]
        return remote(vp, vg.at[buf, i], ag_s.at[i], ag_r.at[buf, i], chip(k, 1))

    def px_copy(par):
        return remote(px, px_in.at[par], px_s, px_r.at[par], chip(0, 1))

    def zg_send(d, par):
        return remote(vp, cz.at[par, p], z_s.at[d], z_r.at[par, p], z_dev(d))

    def zg_recv(d, par):
        o = z_of(d)
        return remote(vp, cz.at[par, o], z_s.at[d], z_r.at[par, o], z_dev(d))

    def rs_copy(d, par):
        return remote(ps.at[z_of(d)], rs.at[par, d], rs_s.at[d], rs_r.at[par, d], (z_of(d), gy, 1 - gz))

    def dt_copy(d, core, par):
        i = 2 * d + core
        return remote(dots_out, dots_in.at[par, i], dt_s.at[i], dt_r.at[par, i], (z_of(d), gy, gz if core == 0 else 1 - gz))

    dot_peers = [(d, core) for d in far_z + [0] for core in range(2) if d + core]

    def dz_copy(d):
        return remote(dsum, dz.at[d], dz_s.at[d], dz_r.at[d], (z_of(d), gy, 1 - gz))

    loads = [
        pltpu.make_async_copy(panels_hbm, panels, in_s.at[0]),
        pltpu.make_async_copy(start_hbm.at[:, own], vp, in_s.at[1]),
        pltpu.make_async_copy(start_hbm, start, in_s.at[2]),
        pltpu.make_async_copy(right_hbm, right, in_s.at[3]),
        pltpu.make_async_copy(diagonal_hbm, diagonal, in_s.at[4]),
    ]
    for load in loads:
        load.start()

    barrier = pltpu.get_barrier_semaphore()
    for k, core in reversed(everyone):
        pl.semaphore_signal(barrier, inc=1, device_id=chip(k, core), device_id_type=MESH)
    for d in far_z:
        for core in range(2):
            dev = (z_of(d), gy, gz if core == 0 else 1 - gz)
            pl.semaphore_signal(barrier, inc=1, device_id=dev, device_id_type=MESH)

    loads[0].wait()

    def split(value):
        top = value.astype(BF16).astype(F32)
        mid = (value - top).astype(BF16).astype(F32)
        return top, mid, value - top - mid

    def other_side(pan, base):
        for s in range(np_):
            here = slice(s * LANE, (s + 1) * LANE)
            ax, ay, at = (pan[i:i + 1, here] for i in range(3))
            other = jnp.where(row8 == 4, 1.0, jnp.where(row8 == 5, ax * ax + ay * ay + at * at, 0.0))
            for i, value in enumerate((ax, ay, at)):
                other = jnp.where(row8 == i, -2.0 * value, other)
            top, mid, low = split(other)
            there = slice(base + s * LANE, base + (s + 1) * LANE)
            rhs[:, there] = jnp.concatenate([top, mid, low, top, mid, top], 0).astype(BF16)

    other_side(panels, 0)

    for load in loads[1:]:
        load.wait()
    for s in range(np_):
        sol_c[s] = start[:, s * LANE:(s + 1) * LANE]
    sums[...] = jnp.zeros_like(sums)
    s_c[...] = jnp.zeros_like(s_c)
    d_c[...] = jnp.zeros_like(d_c)
    r_c[...] = jnp.zeros_like(r_c)
    s_r[...] = jnp.zeros_like(s_r)
    r_r[...] = jnp.zeros_like(r_r)
    zdir[...] = jnp.zeros_like(zdir)
    gprev[...] = jnp.ones_like(gprev)
    aprev[...] = jnp.ones_like(aprev)
    hist[...] = jnp.zeros_like(hist)

    with jax.named_scope("barrier"):
        pl.semaphore_wait(barrier, 2 * ngy - 1 + 2 * (np_ - 1))
    partner_copy().start()
    for k in reversed(every_chip):
        pan_copy(k).start()

    def send_piece(buf):
        for k in every_chip:
            ag_copy(k, buf).start()

    send_piece(0)
    partner_copy().wait_recv()
    other_side(partner, cols_all)

    def build(first, stop):
        for i in range(first, stop):
            pan = rowpan[i]
            ax, ay, at = (pan[j:j + 1] for j in range(3))
            tile = jnp.where(row8 == 4, ax * ax + ay * ay + at * at + SOFT_SQ, jnp.where(row8 == 5, 1.0, 0.0))
            for j, value in enumerate((ax, ay, at)):
                tile = jnp.where(row8 == j, value, tile)
            top, mid, low = split(tile)
            lhs = jnp.concatenate([top, top, top, mid, mid, low], 0).T.astype(BF16)
            there = slice(i * LANE, (i + 1) * LANE)
            for t in range(2 * cols_all // width):
                cols = slice(t * width, (t + 1) * width)
                value = lax.rsqrt(jnp.dot(lhs, rhs[:, cols], preferred_element_type=F32))
                top = value.astype(BF16)
                ghi[there, cols] = top
                glo[there, cols] = (value - top.astype(F32)).astype(BF16)

    width = 2 * LANE

    def pack_dots(parts):
        out = jnp.zeros((8, LANE), F32)
        for d in range(3):
            for g in range(groups):
                out = jnp.where(lane8 == groups * d + g, parts[d][8 * g:8 * g + 8, :], out)
        return out

    def unpack_dots(got):
        out = []
        for d in range(3):
            out.append(jnp.concatenate([got[:, groups * d + g:groups * d + g + 1] for g in range(groups)], 0))
        return out

    def row_sum(value):
        return jnp.sum(value, axis=1, keepdims=True)

    def coefficients(got, turn):
        gamma, delta, omega = unpack_dots(got)
        hist[...] = jnp.where(lane == turn, jnp.sqrt(omega / gamma), hist[...])
        gamma_prev = gprev[:, 0:1]
        alpha_prev = aprev[:, 0:1]
        beta = jnp.where(turn == 0, 0.0, gamma / gamma_prev)
        alpha = gamma / (delta - beta * gamma / alpha_prev)
        gprev[...] = jnp.broadcast_to(gamma, (cases, LANE))
        aprev[...] = jnp.broadcast_to(alpha, (cases, LANE))
        scal[...] = jnp.broadcast_to(beta, (cases, LANE))
        return alpha, beta

    def rows_of(c, buf):
        pieces = []
        for i in range(bounds[c], bounds[c + 1]):
            value = vg[buf, i] * (rowpan[i, 3:4, :] * inv_root)
            top = value.astype(BF16)
            value = value - top.astype(F32)
            mid = value.astype(BF16)
            low = (value - mid.astype(F32)).astype(BF16)
            pieces.append(jnp.concatenate([top, mid, low], 0))
        return jnp.concatenate(pieces, 1)

    def product(lhs, top, low):
        main = jnp.dot(lhs, top, preferred_element_type=F32)
        rest = jnp.dot(lhs[:2 * cases], low, preferred_element_type=F32)
        small = main[2 * cases:] + rest[cases:]
        return main[:cases] + (main[cases:2 * cases] + rest[:cases] + small)

    def matmul(c, buf):
        rows = slice(bounds[c] * LANE, bounds[c + 1] * LANE)
        part = product(rows_of(c, buf), ghi[rows], glo[rows])
        acc[...] = part if c == 0 else part + acc[...]

    def last_product(side_of):
        rows = slice(bounds[nchunk - 1] * LANE, nslot * LANE)
        cols = slice(side_of * cols_all, (side_of + 1) * cols_all)
        return acc[:, cols] + product(lhs_last[...], ghi[rows, cols], glo[rows, cols])

    def dots(first, stop, buf, parts):
        g, d, o = parts
        for i in range(first, stop):
            r, a = r_r[i], vg[buf, i]
            g, d, o = g + r * r, d + a * r, o + a * a
        return g, d, o

    def arrive(c, buf):
        with jax.named_scope(f"ag_wait{c}"):
            for k in order[bounds[c]:bounds[c + 1]]:
                ag_copy(k, buf).wait_recv()

    with jax.named_scope("build"):
        for c in range(nchunk):
            with jax.named_scope(f"pan_wait{c}"):
                first = bounds[c]
                if c == 0:
                    pan_copy(0).wait_recv()
                    build(0, 1)
                    first = 1
                for k in order[first:bounds[c + 1]]:
                    pan_copy(k).wait_recv()
            if c > 0:
                arrive(c - 1, 0)
            build(first, bounds[c + 1])
            if c > 0:
                matmul(c - 1, 0)
    partner_copy().wait_send()
    for k in every_chip:
        pan_copy(k).wait_send()

    def event(e, carry):
        par = lax.rem(e, 2)
        nxt = 1 - par
        buf = lax.rem(e, 3)
        after = lax.rem(e + 1, 3)
        @pl.when(e > 0)
        def _():
            for c in range(nchunk - 1):
                arrive(c, buf)
                with jax.named_scope(f"matmul{c}"):
                    matmul(c, buf)
                    parts = (sums[0], sums[1], sums[2])
                    if c == 0:
                        parts = (jnp.zeros((cases, LANE), F32),) * 3
                    sums[0], sums[1], sums[2] = dots(bounds[c], bounds[c + 1], buf, parts)
        arrive(nchunk - 1, buf)
        with jax.named_scope("last_A"):
            lhs_last[...] = rows_of(nchunk - 1, buf)
            part = last_product(0)
            for s in range(np_):
                px[s] = part[:, s * LANE:(s + 1) * LANE]
            parts = dots(bounds[nchunk - 1], nslot, buf, (sums[0], sums[1], sums[2]))
            dots_out[...] = pack_dots([row_sum(v) for v in parts])
        px_copy(par).start()

        @pl.when(e >= 2)
        def _():
            for d, core in dot_peers:
                dt_copy(d, core, par).start()
        with jax.named_scope("last_B"):
            part = last_product(1)
            for s in range(np_):
                ps[s] = part[:, s * LANE:(s + 1) * LANE]
        dots_in[par, 0] = dots_out[...]
        with jax.named_scope("px_wait"):
            px_copy(par).wait_recv()
        for d in far_z + [0]:
            to = z_of(d)
            ps[to] = ps[to] + px_in[par, to]
            rs_copy(d, par).start()
        px_copy(par).wait_send()
        for k in every_chip:
            ag_copy(k, buf).wait_send()

        @pl.when(e > 0)
        def _():
            for d in far_z:
                zg_send(d, par).wait_send()
            cz[par, p] = vp[...]
        with jax.named_scope("rs_wait"):
            @pl.when(e >= 2)
            def _():
                for d, core in dot_peers:
                    dt_copy(d, core, par).wait_recv()
                coefficients(jnp.sum(dots_in[par], axis=0), e - 2)
            for d in far_z + [0]:
                rs_copy(d, par).wait_recv()
        got = jnp.sum(rs[par], axis=0)
        fresh = got * panels[3:4, own] + diagonal[0:1, own] * vp[...]

        @pl.when(e == 0)
        def _():
            vp[...] = right[:, own] - fresh

        @pl.when(e == 1)
        def _():
            vp[...] = fresh

        @pl.when(e >= 2)
        def _():
            z = fresh + scal[...] * zdir[...]
            zdir[...] = z
            vp[...] = vp[...] - aprev[...] * z

        @pl.when(e < ITERS)
        def _():
            send_piece(after)
        for d in far_z:
            zg_send(d, nxt).start()
        with jax.named_scope("rs_send"):
            for d in far_z + [0]:
                rs_copy(d, par).wait_send()

        @pl.when(e >= 2)
        def _():
            for d, core in dot_peers:
                dt_copy(d, core, par).wait_send()

        @pl.when(e > 0)
        def _():
            for d in far_z:
                zg_recv(d, par).wait_recv()

        @pl.when(e == 1)
        def _():
            loop(0, nslot, lambda s: r_r.__setitem__(s, vg[buf, s]))
            loop(0, np_, lambda s: r_c.__setitem__(s, cz[par, s]))

        @pl.when(e >= 2)
        def _():
            alpha = aprev[...]
            beta = scal[...]

            def rows(s):
                step = vg[buf, s] + beta * s_r[s]
                s_r[s] = step
                r_r[s] = r_r[s] - alpha * step
            loop(0, jnp.where(e < ITERS, nslot, 0), rows)

            def cols(s):
                step = cz[par, s] + beta * s_c[s]
                s_c[s] = step
                along = r_c[s] + beta * d_c[s]
                d_c[s] = along
                sol_c[s] = sol_c[s] + alpha * along
                r_c[s] = r_c[s] - alpha * step
            loop(0, np_, cols)
        return carry

    lax.fori_loop(0, ITERS + 1, event, 0)

    last = (ITERS + 1) % 2
    r = r_c[p]
    a = vp[...]
    dtile[...] = pack_dots([row_sum(r * r), row_sum(a * r), row_sum(a * a)])
    for k, core in reversed(everyone):
        plane_copy(k, core).start()
    dplane[0] = dtile[...]
    cz[last, p] = vp[...]
    with jax.named_scope("dp_wait"):
        for k, core in everyone:
            plane_copy(k, core).wait_recv()
    dsum[...] = jnp.sum(dplane[...], axis=0)
    for d in far_z:
        dz_copy(d).start()
    dz[0] = dsum[...]
    for k, core in everyone:
        plane_copy(k, core).wait_send()
    for d in far_z:
        zg_send(d, last).wait_send()
    with jax.named_scope("dz_wait"):
        for d in far_z:
            zg_recv(d, last).wait_recv()
        for d in far_z:
            dz_copy(d).wait_recv()
    alpha, beta = coefficients(jnp.sum(dz[...], axis=0), ITERS - 1)
    for s in range(np_):
        cols = slice(s * LANE, (s + 1) * LANE)
        step = cz[last, s] + beta * s_c[s]
        along = r_c[s] + beta * d_c[s]
        sol_out[:, cols] = sol_c[s] + alpha * along
        res_out[:, cols] = r_c[s] - alpha * step
    hist_out[...] = hist[...].T[0:ITERS, :]
    for d in far_z:
        dz_copy(d).wait_send()


def hand_over(*refs):
    n = (len(refs) - 1) // 3
    src, dst, mid, sems = refs[:n], refs[n:2 * n], refs[2 * n:3 * n], refs[3 * n]
    loads = [pltpu.make_async_copy(src[i], mid[i], sems.at[0, i]) for i in range(n)]
    stores = [pltpu.make_async_copy(mid[i], dst[i], sems.at[1, i]) for i in range(n)]
    for load in loads:
        load.start()
    for load, store in zip(loads, stores):
        load.wait()
        store.start()
    for store in stores:
        store.wait()


def on_device(np_, ngy, panels, diagonal, right, start):
    cases, cols = right.shape
    nslot = ngy
    bounds = chunk_bounds(nslot)
    span = LANE * (nslot - bounds[-2])
    vm = lambda *shape: pltpu.VMEM(shape, F32)
    half = lambda *shape: pltpu.VMEM(shape, BF16)
    dma = lambda *shape: pltpu.SemaphoreType.DMA(shape)
    state = (np_, cases, LANE)
    wide = (nslot, cases, LANE)
    one = (cases, LANE)
    scratch = [
        vm(4, cols), vm(4, cols), vm(1, cols), vm(cases, cols), vm(cases, cols), vm(nslot, 4, LANE),
        half(nslot * LANE, 2 * cols), half(nslot * LANE, 2 * cols), half(48, 2 * cols), half(3 * cases, span),
        vm(*one), vm(3, *wide), vm(2, *state), vm(*state), vm(2, *state), vm(*state), vm(2, *state),
        vm(8, LANE), vm(2, 2 * np_, 8, LANE), vm(cases, 2 * cols),
        vm(*state), vm(*state), vm(*state), vm(*state), vm(*wide), vm(*wide),
        vm(*one), vm(*one), vm(*one), vm(*one), vm(*one), vm(3, *one),
        vm(8, LANE), vm(2 * nslot, 8, LANE), vm(8, LANE), vm(np_, 8, LANE),
        dma(5), dma(nslot), dma(nslot), pltpu.SemaphoreType.DMA, pltpu.SemaphoreType.DMA,
        dma(nslot), dma(3, nslot), dma(np_), dma(2, np_), pltpu.SemaphoreType.DMA, dma(2),
        dma(np_), dma(2, np_), dma(2 * np_), dma(2, 2 * np_),
        dma(2 * nslot), dma(2 * nslot), dma(np_), dma(np_),
    ]
    results = pl.pallas_call(
        functools.partial(cg_kernel, np_, ngy, cases),
        out_shape=(
            jax.ShapeDtypeStruct((cases, cols), F32),
            jax.ShapeDtypeStruct((cases, cols), F32),
            jax.ShapeDtypeStruct((ITERS, cases), F32),
        ),
        in_specs=[pl.BlockSpec(memory_space=pltpu.HBM)] * 4,
        out_specs=tuple([pl.BlockSpec(memory_space=pltpu.VMEM)] * 3),
        scratch_shapes=scratch,
        compiler_params=pltpu.CompilerParams(
            collective_id=0, has_side_effects=True, vmem_limit_bytes=60 * 1024 * 1024
        ),
        name="cg",
    )(panels, diagonal[None, :], right, start)
    return pl.pallas_call(
        hand_over,
        out_shape=tuple(jax.ShapeDtypeStruct(r.shape, r.dtype) for r in results),
        in_specs=[pl.BlockSpec(memory_space=pltpu.HBM)] * 3,
        out_specs=tuple([pl.BlockSpec(memory_space=pltpu.HBM)] * 3),
        scratch_shapes=[pltpu.VMEM(r.shape, r.dtype) for r in results] + [pltpu.SemaphoreType.DMA((2, 3))],
        compiler_params=pltpu.CompilerParams(vmem_limit_bytes=60 * 1024 * 1024),
        name="hand_over",
    )(*results)


def solution(mesh):
    cut = P(None, ("gy", "gz"))
    sizes = dict(mesh.shape)
    return jax.shard_map(
        functools.partial(on_device, sizes["gx"], sizes["gy"]),
        mesh=mesh,
        in_specs=(cut, P(("gy", "gz")), cut, cut),
        out_specs=(cut, cut, P()),
        check_vma=False,
    )
```
